128 devices in a mesh: blk: 64 (over z_lo, x, y, core), slab: 2 (over z_hi).
Axes of the slice: x: 4, y: 4, z: 4 (z_hi: 2, z_lo: 2; z = z_hi * 2 + z_lo), core: 2. Of those that a mesh axis runs over, the one named last changes fastest.
Arguments:
- sinogram: bfloat16 [128, 8, 2048], P('blk', 'slab'), parts along dimension 1, may hold values from -6 to 6
- jitter: bfloat16 [128], P('blk'), may hold values from -0.29882812 to 0.29882812
- shift: int32 [128], replicated, may hold values from -8 to 8
Outputs:
- image: float32 [128, 8, 2048], P('blk', 'slab'), parts along dimension 1
The draws below stay inside these ranges and needn't reach their ends.
There are 2 independent parts, one for each index of `slab`. The reference program is written for one: setup_inputs(seed, part) draws one part's arguments, and reference() takes and returns one part's arrays. A program takes and returns all parts, laid end to end along the dimension named above; an argument that names none is the same for every part. Nothing has to cross between parts.
All inputs are finite; a program needn't handle non-finite values.
Results may differ from the reference program's by a relative error of at most 0.0055.
Values may be sent and summed in bfloat16 or wider, within the bound.
A program may use at most 64 MiB of HBM per device.

```python
import math
import jax
import jax.numpy as jnp
from jax import lax

BINS = 2048
SLICES = 4
ANGLES = 128
NROWS = 128


def place_ends(array, rng, smallest, top_value):
    index_at = [jax.random.randint(jax.random.fold_in(rng, axis), (), 0, length) for axis, length in enumerate(array.shape)]
    main_axis = array.shape.index(max(array.shape))
    beside = index_at[:main_axis] + [(index_at[main_axis] + 1) % array.shape[main_axis]] + index_at[main_axis + 1:]
    return array.at[tuple(index_at)].set(smallest).at[tuple(beside)].set(top_value)


def block_scale(rng, shape, split, smallest, high):
    def one(dim, shards_of):
        heights = jax.random.uniform(jax.random.fold_in(jax.random.fold_in(rng, 6), dim), (shards_of,), jnp.float32, smallest / len(split), high / len(split))
        return jnp.repeat(jnp.exp(heights), shape[dim] // shards_of).reshape((-1,) + (1,) * (len(shape) - dim - 1))

    level = one(*split[0])
    for cut in split[1:]:
        level = level * one(*cut)
    return level


def bell_draw(key, shape, deviation, most, pieces=(), held_as=jnp.bfloat16):
    entries = deviation * jax.random.normal(key, shape, jnp.float32)
    if pieces:
        entries = entries * block_scale(key, shape, pieces, -0.22, 0.18)
    return jnp.clip(entries, -most, most).astype(held_as)


def setup_inputs(seed: int = 0, part: int = 0) -> dict:
    splits = jax.random.split(jax.random.key(seed), 4)
    part_keys = jax.random.split(jax.random.fold_in(splits[3], part), 4)
    return {
        "sinogram": bell_draw(part_keys[0], (ANGLES, SLICES, BINS), 1.0, 6.0, ((0, 64),)),
        "jitter": jnp.clip(jax.random.uniform(splits[1], (ANGLES,), jnp.float32, -0.29882812, 0.29882812) * block_scale(splits[1], (ANGLES,), ((0, 64),), -0.4, 0.0), -0.29882812, 0.29882812).astype(jnp.bfloat16),
        "shift": place_ends(jax.random.randint(splits[2], (ANGLES,), -8, 9), jax.random.fold_in(splits[2], 1), -8, 8).astype(jnp.int32),
    }


def ramp_matrix(bins):
    offsets = jnp.arange(bins, dtype=jnp.int32)[None, :] - jnp.arange(bins, dtype=jnp.int32)[:, None]
    safe = jnp.where(offsets == 0, 1, offsets).astype(jnp.float32)
    odd_part = jnp.where(offsets % 2 != 0, -1.0 / (math.pi ** 2 * safe * safe), jnp.float32(0.0))
    kernel = jnp.where(offsets == 0, jnp.float32(0.25), odd_part)
    return kernel.astype(jnp.bfloat16)

def reference(sinogram, jitter, shift):
    ramp = ramp_matrix(BINS)
    jit_vals = jitter.astype(jnp.float32)
    weight = (1.0 + (jnp.roll(jit_vals, -1) - jnp.roll(jit_vals, 1)) * 1.5) * (4.0 / math.sqrt(ANGLES))
    flat = jnp.dot(sinogram.reshape(ANGLES * SLICES, BINS), ramp, preferred_element_type=jnp.float32)
    filtered = (flat.reshape(ANGLES, SLICES, BINS) * weight[:, None, None]).astype(jnp.bfloat16)
    padding = BINS // 4 + 192
    padded = jnp.pad(filtered, ((0, 0), (0, 0), (padding, padding))).astype(jnp.float32)
    theta = (jnp.arange(ANGLES, dtype=jnp.float32) + jit_vals) * math.pi / ANGLES
    cosine = jnp.cos(theta)
    sine_part = jnp.sin(theta)
    center_bin = (BINS - 1) / 2 + shift.astype(jnp.float32)
    coords_x = jnp.arange(BINS, dtype=jnp.float32) - (BINS - 1) / 2

    def one_row(row):
        row_pos = row.astype(jnp.float32) - (NROWS - 1) / 2
        coords = coords_x[None, :] * cosine[:, None] + row_pos * sine_part[:, None] + center_bin[:, None]
        lower = jnp.floor(coords)
        upper = lower + 1.0
        w_lower = jnp.maximum(0.0, 1.0 - jnp.abs(lower - coords)).astype(jnp.bfloat16).astype(jnp.float32)
        w_upper = jnp.maximum(0.0, 1.0 - jnp.abs(upper - coords)).astype(jnp.bfloat16).astype(jnp.float32)
        low_idx = lower.astype(jnp.int32) + padding
        idx_lo = jnp.broadcast_to(low_idx[:, None, :], (ANGLES, SLICES, BINS))
        f_lower = jnp.take_along_axis(padded, idx_lo, axis=2)
        f_upper = jnp.take_along_axis(padded, idx_lo + 1, axis=2)
        return lax.optimization_barrier(jnp.sum(f_lower * w_lower[:, None, :] + f_upper * w_upper[:, None, :], axis=0))
    return lax.map(one_row, jnp.arange(NROWS, dtype=jnp.int32))
```

```python
import functools
import math

import jax
import jax.numpy as jnp
from jax import lax
from jax.experimental import pallas as pl
from jax.experimental.pallas import tpu as pltpu
from jax.sharding import PartitionSpec as P

BINS = 2048
ANGLES = 128
NROWS = 128
TILES = 18
STRIP = 3968
F32 = jnp.float32
BF16 = jnp.bfloat16


def hop(r):
    dz = jnp.where((r == 0) | (r == 1) | (r == 2) | (r == 6), 0, 1)
    dx = jnp.where(
        (r == 0) | (r == 3), 0, jnp.where((r == 1) | (r == 4), 1, jnp.where((r == 2) | (r == 5), 3, 2))
    )
    return dz, dx


def source_of(m, r):
    dz, dx = hop(r)
    return ((m // 4 + dz) % 2) * 4 + (m % 4 + 4 - dx) % 4


def target_of(m, r):
    dz, dx = hop(r)
    return ((m // 4 + dz) % 2) * 4 + (m % 4 + dx) % 4


def lane_gather(x, idx):
    return jnp.take_along_axis(x, idx, axis=1, mode="promise_in_bounds")


def build_strip(strip):
    shape = (128, 128)
    diff = lax.broadcasted_iota(jnp.int32, shape, 1) - lax.broadcasted_iota(jnp.int32, shape, 0)
    odd = (diff % 2) != 0
    diff_f = diff.astype(F32)

    def chunk(c, _):
        n = diff_f + (1920 - 128 * c).astype(F32)
        value = jnp.where(odd, (-1.0 / math.pi**2) / (n * n), 0.0)
        value = jnp.where(n == 0.0, 0.25, value)
        strip[pl.ds(pl.multiple_of(c * 128, 128), 128), :] = value.astype(BF16)
        return 0

    lax.fori_loop(0, STRIP // 128, chunk, 0)


def filter_rows(sino, strip, flat, msg):
    x = jnp.concatenate([sino[0].astype(F32), sino[1].astype(F32)], axis=0)
    xs = jnp.concatenate([x[:, 256 * i : 256 * i + 256] for i in range(8)], axis=0).astype(BF16)
    for d in range(-7, 8):
        rhs = jnp.concatenate(
            [strip[1920 - 128 * e : 1920 - 128 * e + 256, :] for e in (2 * d, 2 * d + 1)], axis=1
        )
        part = jnp.dot(xs, rhs, preferred_element_type=F32)
        for i in range(max(0, -d), min(8, 8 - d)):
            j = i + d
            piece = part[8 * i : 8 * i + 8, :]
            if i == 7:
                flat[8 * j : 8 * j + 8, :] = piece
            else:
                flat[8 * j : 8 * j + 8, :] += piece
    for j in range(8):
        msg[0, :, 256 * j : 256 * j + 256] = flat[8 * j : 8 * j + 8, :].astype(BF16)


def kernel(
    sino, jit, shift, out,
    strip, flat, msg, jr, fbuf, dbuf, tab, tabi, stab, stabi, acc, turn, sendb, recvb,
    jsend, jrecv, msend, mrecv, rsend, rrecv, tsem,
):
    idx = lax.axis_index("blk")
    m = idx // 8
    j = idx % 8
    barrier = pltpu.get_barrier_semaphore()

    def device(mm, jj):
        return {"blk": mm * 8 + jj}

    for dj in (-1, 0, 1):
        for r in range(8):
            if dj == 0 and r == 0:
                continue
            pl.semaphore_signal(barrier, inc=1, device_id=device(target_of(m, r), (j + dj + 8) % 8))
    for dj in (2, 3, 4, 5, 6):
        pl.semaphore_signal(barrier, inc=1, device_id=device(m, (j + dj) % 8))

    lane1 = lax.broadcasted_iota(jnp.int32, (1, 128), 1)
    second1 = ((lane1 // 32) == 1) | ((lane1 // 32) == 2)
    jv = jit[...].astype(F32)
    jrow = jnp.where(second1, jnp.broadcast_to(jv[:, 1:2], (1, 128)), jnp.broadcast_to(jv[:, 0:1], (1, 128)))
    jr[8] = jrow

    build_strip(strip)
    filter_rows(sino, strip, flat, msg)

    pl.semaphore_wait(barrier, 28)

    jcopies = []
    for dj in (-1, 0, 1):
        jj = (j - dj + 8) % 8
        base = m if dj == 0 else (jnp.where(j == 0, (m + 7) % 8, m) if dj == 1 else jnp.where(j == 7, (m + 1) % 8, m))
        for r in range(8):
            if dj == 0 and r == 0:
                continue
            slot = (dj + 1) * 8 + r
            jcopies.append(
                pltpu.make_async_remote_copy(
                    src_ref=jr.at[8], dst_ref=jr.at[slot],
                    send_sem=jsend.at[slot], recv_sem=jrecv.at[slot],
                    device_id=device(target_of(base, r), jj),
                )
            )
    for c in jcopies:
        c.start()
    mcopies = []
    for r in range(1, 8):
        mcopies.append(
            pltpu.make_async_remote_copy(
                src_ref=msg.at[0], dst_ref=msg.at[r],
                send_sem=msend.at[r], recv_sem=mrecv.at[r],
                device_id=device(target_of(m, r), j),
            )
        )
    for c in mcopies:
        c.start()

    for c in jcopies:
        c.wait_recv()
    shape = (8, 128)
    lane = lax.broadcasted_iota(jnp.int32, shape, 1)
    sub = lax.broadcasted_iota(jnp.int32, shape, 0)
    a_l = (lane // 32) % 2
    g_l = (lane // 16) % 2
    k_l = lane % 16

    def rows_of(start):
        return jnp.concatenate([jr[start + r] for r in range(8)], axis=0)

    here = rows_of(8)
    before = pltpu.roll(rows_of(0), 64, 1)
    after = pltpu.roll(rows_of(16), 64, 1)
    other = pltpu.roll(here, 64, 1)
    nxt = jnp.where(a_l == 0, other, after)
    prv = jnp.where(a_l == 1, other, before)
    weight = (1.0 + (nxt - prv) * 1.5) * (4.0 / math.sqrt(ANGLES))
    angle = source_of(m, sub) * 16 + 2 * j + a_l
    theta = (angle.astype(F32) + here) * math.pi / ANGLES
    cosine = jnp.cos(theta)
    sine = jnp.sin(theta)
    offset = lane_gather(jnp.broadcast_to(shift[...], shape), angle).astype(F32)
    center = (
        cosine * (128.0 * k_l.astype(F32) - (BINS - 1) / 2)
        + sine * ((16 * m + 8 * g_l).astype(F32) - (NROWS - 1) / 2)
        + ((BINS - 1) / 2 + 128.0 + offset)
    )
    lowest = center + jnp.minimum(0.0, 127.0 * cosine) + jnp.minimum(0.0, 7.0 * sine) - 0.01
    tile_f = jnp.floor(lowest * (1.0 / 128.0))
    tab[0] = center - 128.0 * tile_f
    tab[1] = weight
    tab[2] = cosine
    tab[3] = sine
    tabi[...] = jnp.clip(tile_f.astype(jnp.int32), 0, TILES - 2)
    tc = pltpu.make_async_copy(tab, stab, tsem.at[0])
    ti = pltpu.make_async_copy(tabi, stabi, tsem.at[1])
    tc.start()
    ti.start()
    acc[...] = jnp.zeros_like(acc)
    tc.wait()
    ti.wait()

    last = lane == 127
    lane_f = lane.astype(F32)
    sub_f = sub.astype(F32)
    zero = jnp.zeros(shape, F32)

    def one_source(r, _):
        @pl.when(r > 0)
        def _():
            pltpu.make_async_copy(msg.at[r], msg.at[r], mrecv.at[r]).wait()

        w = jnp.where(sub < 4, stab[1, r, 0], stab[1, r, 32])
        base = r * (TILES * 8)

        def put(ref, t, value):
            ref[pl.ds(pl.multiple_of(base + t * 8, 8), 8), :] = value

        prev, prev_rolled = zero, zero
        put(fbuf, 0, zero)
        for t in range(1, TILES):
            if t < TILES - 1:
                f = msg[r, :, 128 * (t - 1) : 128 * t].astype(F32) * w
                rolled = pltpu.roll(f, 127, 1)
            else:
                f, rolled = zero, zero
            put(fbuf, t, f)
            put(dbuf, t - 1, jnp.where(last, rolled, prev_rolled) - prev)
            prev, prev_rolled = f, rolled
        put(dbuf, TILES - 1, zero)

        ramps = [stab[2, r, 32 * a] * lane_f + stab[3, r, 32 * a] * sub_f for a in range(2)]

        def one_group(g, _):
            for k in range(16):
                total = [acc[g, k, s] for s in range(4)]
                for a in range(2):
                    col = 32 * a + 16 * g + k
                    v = ramps[a] + stab[0, r, col]
                    row = base + stabi[r, col] * 8 + 4 * a
                    cell = v.astype(jnp.int32)
                    frac = v - cell.astype(F32)
                    upper = cell >= 128
                    pick = cell & 127
                    for s in range(4):
                        def at(ref, shift_rows):
                            one = ref[pl.ds(row + (s + shift_rows), 1), :]
                            return lane_gather(jnp.broadcast_to(one, shape), pick)

                        f = jnp.where(upper, at(fbuf, 8), at(fbuf, 0))
                        d = jnp.where(upper, at(dbuf, 8), at(dbuf, 0))
                        total[s] = total[s] + (f + frac * d)
                for s in range(4):
                    acc[g, k, s] = total[s]
            return 0

        lax.fori_loop(0, 2, one_group, 0)
        return 0

    lax.fori_loop(0, 8, one_source, 0)

    for g in range(2):
        for k in range(16):
            for s in range(4):
                turn[g, k, pl.ds(s, 8, stride=4), :] = acc[g, k, s]
    for g in range(2):
        for q in range(4):
            for k in range(16):
                sendb[4 * g + q, :, 128 * k : 128 * k + 128] = turn[g, k, 8 * q : 8 * q + 8, :].astype(BF16)
    rcopies = []
    for dj in range(1, 8):
        jj = (j + dj) % 8
        rcopies.append(
            pltpu.make_async_remote_copy(
                src_ref=sendb.at[jj], dst_ref=recvb.at[dj],
                send_sem=rsend.at[dj], recv_sem=rrecv.at[dj],
                device_id=device(m, jj),
            )
        )
    for c in rcopies:
        c.start()
    for c in rcopies:
        c.wait_recv()
    g_own, q_own = j // 4, j % 4
    for k in range(16):
        total = turn[g_own, k, pl.ds(pl.multiple_of(q_own * 8, 8), 8), :]
        for dj in range(1, 8):
            total = total + recvb[dj, :, 128 * k : 128 * k + 128].astype(F32)
        out[:, 128 * k : 128 * k + 128] = total
    for c in jcopies + mcopies + rcopies:
        c.wait_send()


def body(sinogram, jitter, shift):
    vmem = pl.BlockSpec(memory_space=pltpu.VMEM)
    image = pl.pallas_call(
        kernel,
        out_shape=jax.ShapeDtypeStruct((8, BINS), F32),
        in_specs=[vmem] * 3,
        out_specs=vmem,
        scratch_shapes=[
            pltpu.VMEM((STRIP, 128), BF16),
            pltpu.VMEM((64, 256), F32),
            pltpu.VMEM((8, 8, BINS), BF16),
            pltpu.VMEM((24, 1, 128), F32),
            pltpu.VMEM((8 * TILES * 8, 128), F32),
            pltpu.VMEM((8 * TILES * 8, 128), F32),
            pltpu.VMEM((4, 8, 128), F32),
            pltpu.VMEM((8, 128), jnp.int32),
            pltpu.SMEM((4, 8, 128), F32),
            pltpu.SMEM((8, 128), jnp.int32),
            pltpu.VMEM((2, 16, 4, 8, 128), F32),
            pltpu.VMEM((2, 16, 32, 128), F32),
            pltpu.VMEM((8, 8, BINS), BF16),
            pltpu.VMEM((8, 8, BINS), BF16),
            pltpu.SemaphoreType.DMA((24,)),
            pltpu.SemaphoreType.DMA((24,)),
            pltpu.SemaphoreType.DMA((8,)),
            pltpu.SemaphoreType.DMA((8,)),
            pltpu.SemaphoreType.DMA((8,)),
            pltpu.SemaphoreType.DMA((8,)),
            pltpu.SemaphoreType.DMA((2,)),
        ],
        compiler_params=pltpu.CompilerParams(collective_id=0, has_side_effects=True),
    )(sinogram, jitter.reshape(1, 2), shift.reshape(1, 128))
    return image.reshape(2, 4, BINS)


def solution(mesh):
    return jax.shard_map(
        body,
        mesh=mesh,
        in_specs=(P("blk", "slab", None), P("blk"), P()),
        out_specs=P("blk", "slab", None),
        check_vma=False,
    )
```

```python
import functools
import math

import jax
import jax.numpy as jnp
from jax import lax
from jax.experimental import pallas as pl
from jax.experimental.pallas import tpu as pltpu
from jax.sharding import PartitionSpec as P

BINS = 2048
ANGLES = 128
NROWS = 128
TILES = 18
STRIP = 3968
ROWS = 8 * TILES * 16
F32 = jnp.float32
BF16 = jnp.bfloat16


def hop(r):
    dz = jnp.where((r == 0) | (r == 1) | (r == 2) | (r == 6), 0, 1)
    dx = jnp.where(
        (r == 0) | (r == 3), 0, jnp.where((r == 1) | (r == 4), 1, jnp.where((r == 2) | (r == 5), 3, 2))
    )
    return dz, dx


def source_of(m, r):
    dz, dx = hop(r)
    return ((m // 4 + dz) % 2) * 4 + (m % 4 + 4 - dx) % 4


def target_of(m, r):
    dz, dx = hop(r)
    return ((m // 4 + dz) % 2) * 4 + (m % 4 + dx) % 4


def lane_gather(x, idx):
    dims = lax.GatherDimensionNumbers(
        offset_dims=(),
        collapsed_slice_dims=(1,),
        start_index_map=(1,),
        operand_batching_dims=(0,),
        start_indices_batching_dims=(0,),
    )
    return lax.gather(
        x, idx[:, :, None], dims, slice_sizes=(1, 1), mode=lax.GatherScatterMode.PROMISE_IN_BOUNDS
    )


def build_strip(strip):
    shape = (128, 128)
    diff = lax.broadcasted_iota(jnp.int32, shape, 1) - lax.broadcasted_iota(jnp.int32, shape, 0)
    odd = (diff % 2) != 0
    diff_f = diff.astype(F32)

    def chunk(c, _):
        n = diff_f + (1920 - 128 * c).astype(F32)
        value = jnp.where(odd, (-1.0 / math.pi**2) / (n * n), 0.0)
        value = jnp.where(n == 0.0, 0.25, value)
        strip[pl.ds(pl.multiple_of(c * 128, 128), 128), :] = value.astype(BF16)
        return 0

    lax.fori_loop(0, STRIP // 128, chunk, 0)


def filter_rows(sino, strip, flat, msg):
    x = jnp.concatenate([sino[0].astype(F32), sino[1].astype(F32)], axis=0)
    xs = jnp.concatenate([x[:, 256 * i : 256 * i + 256] for i in range(8)], axis=0).astype(BF16)
    for d in range(-7, 8):
        rhs = jnp.concatenate(
            [strip[1920 - 128 * e : 1920 - 128 * e + 256, :] for e in (2 * d, 2 * d + 1)], axis=1
        )
        part = jnp.dot(xs, rhs, preferred_element_type=F32)
        for i in range(max(0, -d), min(8, 8 - d)):
            j = i + d
            piece = part[8 * i : 8 * i + 8, :]
            if i == 7:
                flat[8 * j : 8 * j + 8, :] = piece
            else:
                flat[8 * j : 8 * j + 8, :] += piece
    for j in range(8):
        msg[0, :, 256 * j : 256 * j + 256] = flat[8 * j : 8 * j + 8, :].astype(BF16)


def kernel(
    sino, jit, shift, out,
    strip, flat, msg, jr, taps, tsrc, isrc, stab, itab, acc, turn, sendb, recvb,
    jsend, jrecv, tsend, trecv, isend, irecv, msend, mrecv, rsend, rrecv,
):
    idx = lax.axis_index("blk")
    m = idx // 8
    j = idx % 8
    barrier = pltpu.get_barrier_semaphore()
    shape = (8, 128)
    lane = lax.broadcasted_iota(jnp.int32, shape, 1)
    sub = lax.broadcasted_iota(jnp.int32, shape, 0)
    lane_f = lane.astype(F32)
    sub_f = sub.astype(F32)
    zero = jnp.zeros(shape, F32)

    def device(mm, jj):
        return {"blk": mm * 8 + jj}

    for dj in (-1, 0, 1):
        for r in range(8):
            if dj == 0 and r == 0:
                continue
            pl.semaphore_signal(barrier, inc=1, device_id=device(target_of(m, r), (j + dj + 8) % 8))
    for dj in (2, 3, 4, 5, 6):
        pl.semaphore_signal(barrier, inc=1, device_id=device(m, (j + dj) % 8))

    jv = jit[...].astype(F32)
    jr[8] = jnp.concatenate([jnp.broadcast_to(jv[:, a : a + 1], (1, 128)) for a in range(2)], axis=0)

    a_l = (lane // 32) % 2
    g_l = (lane // 16) % 2
    k_l = lane % 16
    own_jit = jnp.where(a_l == 0, jnp.broadcast_to(jv[:, 0:1], shape), jnp.broadcast_to(jv[:, 1:2], shape))
    angle = m * 16 + 2 * j + a_l
    theta = (angle.astype(F32) + own_jit) * math.pi / ANGLES
    cosine = jnp.cos(theta)
    sine = jnp.sin(theta)
    offset = lane_gather(jnp.broadcast_to(shift[...], shape), angle).astype(F32)
    center = (
        cosine * (128.0 * k_l.astype(F32) - (BINS - 1) / 2)
        + sine * ((16 * target_of(m, sub) + 8 * g_l).astype(F32) - (NROWS - 1) / 2)
        + ((BINS - 1) / 2 + 128.0 + offset)
    )
    lowest = center + jnp.minimum(0.0, 127.0 * cosine) + jnp.minimum(0.0, 7.0 * sine) - 0.01
    tile_f = jnp.clip(jnp.floor(lowest * (1.0 / 128.0)), 0.0, TILES - 2.0)
    base_f = center - 128.0 * tile_f
    first_row = (sub * TILES + tile_f.astype(jnp.int32)) * 16 + 4 * a_l
    for r in range(8):
        tsrc[r] = jnp.concatenate([x[r : r + 1, :] for x in (base_f, cosine, sine, sine)], axis=0)
        isrc[r] = first_row[r : r + 1, :]
    own_tables = [
        pltpu.make_async_copy(tsrc.at[0], stab.at[0], tsend.at[0]),
        pltpu.make_async_copy(isrc.at[0], itab.at[0], isend.at[0]),
    ]
    for c in own_tables:
        c.start()

    build_strip(strip)
    filter_rows(sino, strip, flat, msg)
    acc[...] = jnp.zeros_like(acc)
    for c in own_tables:
        c.wait()

    pl.semaphore_wait(barrier, 28)

    jcopies = []
    tcopies = []
    mcopies = []
    for dj in (0, -1, 1):
        jj = (j - dj + 8) % 8
        base = m if dj == 0 else (jnp.where(j == 0, (m + 7) % 8, m) if dj == 1 else jnp.where(j == 7, (m + 1) % 8, m))
        for r in range(8):
            if dj == 0 and r == 0:
                continue
            slot = (dj + 1) * 8 + r
            jcopies.append(
                pltpu.make_async_remote_copy(
                    src_ref=jr.at[8], dst_ref=jr.at[slot],
                    send_sem=jsend.at[slot], recv_sem=jrecv.at[slot],
                    device_id=device(target_of(base, r), jj),
                )
            )
    for r in range(1, 8):
        tcopies.append(
            pltpu.make_async_remote_copy(
                src_ref=tsrc.at[r], dst_ref=stab.at[r],
                send_sem=tsend.at[r], recv_sem=trecv.at[r],
                device_id=device(target_of(m, r), j),
            )
        )
        tcopies.append(
            pltpu.make_async_remote_copy(
                src_ref=isrc.at[r], dst_ref=itab.at[r],
                send_sem=isend.at[r], recv_sem=irecv.at[r],
                device_id=device(target_of(m, r), j),
            )
        )
        mcopies.append(
            pltpu.make_async_remote_copy(
                src_ref=msg.at[0], dst_ref=msg.at[r],
                send_sem=msend.at[r], recv_sem=mrecv.at[r],
                device_id=device(target_of(m, r), j),
            )
        )
    for c in jcopies + tcopies + mcopies:
        c.start()
    for c in jcopies:
        c.wait_recv()

    last = lane == 127
    lane_1 = lane_f + 1.0

    def arrive(r):
        @pl.when(r > 0)
        def _():
            pltpu.make_async_copy(msg.at[0], msg.at[0], mrecv.at[r]).wait()
            pltpu.make_async_copy(stab.at[0], stab.at[0], trecv.at[r]).wait()
            pltpu.make_async_copy(itab.at[0], itab.at[0], irecv.at[r]).wait()

    def expand(r):
        own, before, after = jr[8 + r], jr[r], jr[16 + r]
        scale = 4.0 / math.sqrt(ANGLES)
        w0 = (1.0 + (own[1:2, :] - before[1:2, :]) * 1.5) * scale
        w1 = (1.0 + (after[0:1, :] - own[0:1, :]) * 1.5) * scale
        w = jnp.where(sub < 4, jnp.broadcast_to(w0, shape), jnp.broadcast_to(w1, shape))
        base = r * (TILES * 16)

        def put(t, value):
            taps[pl.ds(pl.multiple_of(base + t * 8, 8), 8), :] = value

        prev, prev_rolled = zero, zero
        put(0, zero)
        for t in range(1, TILES):
            if t < TILES - 1:
                f = msg[r, :, 128 * (t - 1) : 128 * t].astype(F32) * w
                rolled = pltpu.roll(f, 127, 1)
            else:
                f, rolled = zero, zero
            put(2 * t, f)
            put(2 * t - 1, jnp.where(last, rolled, prev_rolled) - prev)
            prev, prev_rolled = f, rolled
        put(2 * TILES - 1, zero)

    def ramps_of(r):
        out_r = []
        for a in range(2):
            cos_a, sin_a = stab[r, 1, 32 * a], stab[r, 2, 32 * a]
            step = cos_a * (1.0 - 2e-6)
            rise = sin_a * sub_f
            edge = jnp.where(cos_a >= 0.0, 0.0, 127.0)
            out_r.append((step * lane_f + rise, step * jnp.broadcast_to(edge, shape) + rise))
        return out_r

    def block(r, g, ramps):
        for k in range(16):
            total = [acc[g, k, s] for s in range(4)]
            for a in range(2):
                col = 32 * a + 16 * g + k
                start = stab[r, 0, col]
                row = jnp.clip(itab[r, 0, col], 0, ROWS - 28)
                v = ramps[a][0] + start
                cell = v.astype(jnp.int32)
                frac = v - cell.astype(F32)
                upper = ramps[a][1] + start >= lane_1
                pick = cell & 127
                for s in range(4):
                    def at(o):
                        low = jnp.broadcast_to(taps[pl.ds(row + o, 1), :], shape)
                        high = jnp.broadcast_to(taps[pl.ds(row + (o + 16), 1), :], shape)
                        return lane_gather(jnp.where(upper, high, low), pick)

                    total[s] = total[s] + (at(s) + frac * at(s + 8))
            for s in range(4):
                acc[g, k, s] = total[s]

    g_own, q_own = j // 4, j % 4
    g_far = 1 - g_own
    rcopies = []

    def finish(g, qs):
        for k in range(16):
            for s in range(4):
                turn[g, k, pl.ds(s, 8, stride=4), :] = acc[g, k, s]
        for q in range(4):
            for k in range(16):
                sendb[4 * g + q, :, 128 * k : 128 * k + 128] = turn[g, k, 8 * q : 8 * q + 8, :].astype(BF16)
        for q in qs:
            jj = 4 * g + q
            dj = (jj - j + 8) % 8
            c = pltpu.make_async_remote_copy(
                src_ref=sendb.at[jj], dst_ref=recvb.at[dj],
                send_sem=rsend.at[dj], recv_sem=rrecv.at[dj],
                device_id=device(m, jj),
            )
            c.start()
            rcopies.append(c)

    def early(r, _):
        arrive(r)
        expand(r)
        ramps = ramps_of(r)
        for g in range(2):
            block(r, g, ramps)
        return 0

    lax.fori_loop(0, 4, early, 0)

    def unpack(r, _):
        arrive(r)
        expand(r)
        return 0

    lax.fori_loop(4, 8, unpack, 0)

    def late(g):
        def step(i, _):
            for r in (4 + 2 * i, 5 + 2 * i):
                block(r, g, ramps_of(r))
            return 0

        lax.fori_loop(0, 2, step, 0)

    late(g_far)
    finish(g_far, range(4))
    late(g_own)
    finish(g_own, [(q_own + i) % 4 for i in (1, 2, 3)])

    for dj in range(1, 8):
        pltpu.make_async_copy(recvb.at[0], recvb.at[0], rrecv.at[dj]).wait()
    for k in range(16):
        total = turn[g_own, k, pl.ds(pl.multiple_of(q_own * 8, 8), 8), :]
        for dj in range(1, 8):
            total = total + recvb[dj, :, 128 * k : 128 * k + 128].astype(F32)
        out[:, 128 * k : 128 * k + 128] = total
    for c in jcopies + tcopies + mcopies + rcopies:
        c.wait_send()


def body(sinogram, jitter, shift):
    vmem = pl.BlockSpec(memory_space=pltpu.VMEM)
    image = pl.pallas_call(
        kernel,
        out_shape=jax.ShapeDtypeStruct((8, BINS), F32),
        in_specs=[vmem] * 3,
        out_specs=vmem,
        scratch_shapes=[
            pltpu.VMEM((STRIP, 128), BF16),
            pltpu.VMEM((64, 256), F32),
            pltpu.VMEM((8, 8, BINS), BF16),
            pltpu.VMEM((24, 2, 128), F32),
            pltpu.VMEM((ROWS, 128), F32),
            pltpu.VMEM((8, 4, 128), F32),
            pltpu.VMEM((8, 1, 128), jnp.int32),
            pltpu.SMEM((8, 4, 128), F32),
            pltpu.SMEM((8, 1, 128), jnp.int32),
            pltpu.VMEM((2, 16, 4, 8, 128), F32),
            pltpu.VMEM((2, 16, 32, 128), F32),
            pltpu.VMEM((8, 8, BINS), BF16),
            pltpu.VMEM((8, 8, BINS), BF16),
            pltpu.SemaphoreType.DMA((24,)),
            pltpu.SemaphoreType.DMA((24,)),
            pltpu.SemaphoreType.DMA((8,)),
            pltpu.SemaphoreType.DMA((8,)),
            pltpu.SemaphoreType.DMA((8,)),
            pltpu.SemaphoreType.DMA((8,)),
            pltpu.SemaphoreType.DMA((8,)),
            pltpu.SemaphoreType.DMA((8,)),
            pltpu.SemaphoreType.DMA((8,)),
            pltpu.SemaphoreType.DMA((8,)),
        ],
        compiler_params=pltpu.CompilerParams(collective_id=0, has_side_effects=True),
    )(sinogram, jitter.reshape(1, 2), shift.reshape(1, 128))
    return image.reshape(2, 4, BINS)


def solution(mesh):
    return jax.shard_map(
        body,
        mesh=mesh,
        in_specs=(P("blk", "slab", None), P("blk"), P()),
        out_specs=P("blk", "slab", None),
        check_vma=False,
    )
```

```python
import functools
import math

import jax
import jax.numpy as jnp
from jax import lax
from jax.experimental import pallas as pl
from jax.experimental.pallas import tpu as pltpu
from jax.sharding import PartitionSpec as P

BINS = 2048
ANGLES = 128
NROWS = 128
TILES = 18
STRIP = 3968
ROWS = 8 * TILES * 8
WIDE = BINS + 128
FULL = 16383.0
TINY = 1e-30
F32 = jnp.float32
BF16 = jnp.bfloat16


def hop(r):
    dz = jnp.where((r == 0) | (r == 1) | (r == 2) | (r == 6), 0, 1)
    dx = jnp.where(
        (r == 0) | (r == 3), 0, jnp.where((r == 1) | (r == 4), 1, jnp.where((r == 2) | (r == 5), 3, 2))
    )
    return dz, dx


def source_of(m, r):
    dz, dx = hop(r)
    return ((m // 4 + dz) % 2) * 4 + (m % 4 + 4 - dx) % 4


def target_of(m, r):
    dz, dx = hop(r)
    return ((m // 4 + dz) % 2) * 4 + (m % 4 + dx) % 4


def lane_gather(x, idx):
    dims = lax.GatherDimensionNumbers(
        offset_dims=(),
        collapsed_slice_dims=(1,),
        start_index_map=(1,),
        operand_batching_dims=(0,),
        start_indices_batching_dims=(0,),
    )
    return lax.gather(
        x, idx[:, :, None], dims, slice_sizes=(1, 1), mode=lax.GatherScatterMode.PROMISE_IN_BOUNDS
    )


def build_strip(strip):
    shape = (128, 128)
    diff = lax.broadcasted_iota(jnp.int32, shape, 1) - lax.broadcasted_iota(jnp.int32, shape, 0)
    odd = (diff % 2) != 0
    diff_f = diff.astype(F32)

    def chunk(c, _):
        n = diff_f + (1920 - 128 * c).astype(F32)
        value = jnp.where(odd, (-1.0 / math.pi**2) / (n * n), 0.0)
        value = jnp.where(n == 0.0, 0.25, value)
        strip[pl.ds(pl.multiple_of(c * 128, 128), 128), :] = value.astype(BF16)
        return 0

    lax.fori_loop(0, STRIP // 128, chunk, 0)


def filter_rows(sino, strip, flat, msg):
    x = jnp.concatenate([sino[0].astype(F32), sino[1].astype(F32)], axis=0)
    xs = jnp.concatenate([x[:, 256 * i : 256 * i + 256] for i in range(8)], axis=0).astype(BF16)
    for d in range(-7, 8):
        rhs = jnp.concatenate(
            [strip[1920 - 128 * e : 1920 - 128 * e + 256, :] for e in (2 * d, 2 * d + 1)], axis=1
        )
        part = jnp.dot(xs, rhs, preferred_element_type=F32)
        for i in range(max(0, -d), min(8, 8 - d)):
            j = i + d
            piece = part[8 * i : 8 * i + 8, :]
            if i == 7:
                flat[8 * j : 8 * j + 8, :] = piece
            else:
                flat[8 * j : 8 * j + 8, :] += piece
    peak = jnp.zeros((8, 128), F32)
    for j in range(8):
        rows = flat[8 * j : 8 * j + 8, :].astype(BF16)
        msg[0, :, 256 * j : 256 * j + 256] = rows
        size = jnp.abs(rows.astype(F32))
        peak = jnp.maximum(peak, jnp.maximum(size[:, :128], size[:, 128:]))
    peak = jnp.broadcast_to(jnp.max(peak, axis=1, keepdims=True), (8, 128))
    peak = jnp.maximum(peak, jnp.concatenate([peak[4:8], peak[0:4]], axis=0))
    msg[0, :, BINS:WIDE] = peak.astype(BF16)


def kernel(
    sino, jit, shift, out,
    strip, flat, msg, jr, taps, unit, alone, tsrc, isrc, stab, itab, acc, turn, sendb, recvb,
    jsend, jrecv, tsend, trecv, isend, irecv, msend, mrecv, rsend, rrecv,
):
    idx = lax.axis_index("blk")
    m = idx // 8
    j = idx % 8
    barrier = pltpu.get_barrier_semaphore()
    shape = (8, 128)
    lane = lax.broadcasted_iota(jnp.int32, shape, 1)
    sub = lax.broadcasted_iota(jnp.int32, shape, 0)
    lane_f = lane.astype(F32)
    sub_f = sub.astype(F32)
    zero = jnp.zeros(shape, F32)

    def device(mm, jj):
        return {"blk": mm * 8 + jj}

    for dj in (-1, 0, 1):
        for r in range(8):
            if dj == 0 and r == 0:
                continue
            pl.semaphore_signal(barrier, inc=1, device_id=device(target_of(m, r), (j + dj + 8) % 8))
    for dj in (2, 3, 4, 5, 6):
        pl.semaphore_signal(barrier, inc=1, device_id=device(m, (j + dj) % 8))

    jv = jit[...].astype(F32)
    jr[8] = jnp.concatenate([jnp.broadcast_to(jv[:, a : a + 1], (1, 128)) for a in range(2)], axis=0)

    a_l = (lane // 32) % 2
    g_l = (lane // 16) % 2
    k_l = lane % 16
    own_jit = jnp.where(a_l == 0, jnp.broadcast_to(jv[:, 0:1], shape), jnp.broadcast_to(jv[:, 1:2], shape))
    angle = m * 16 + 2 * j + a_l
    theta = (angle.astype(F32) + own_jit) * math.pi / ANGLES
    cosine = jnp.cos(theta)
    sine = jnp.sin(theta)
    offset = lane_gather(jnp.broadcast_to(shift[...], shape), angle).astype(F32)
    center = (
        cosine * (128.0 * k_l.astype(F32) - (BINS - 1) / 2)
        + sine * ((16 * target_of(m, sub) + 8 * g_l).astype(F32) - (NROWS - 1) / 2)
        + ((BINS - 1) / 2 + 128.0 + offset)
    )
    lowest = center + jnp.minimum(0.0, 127.0 * cosine) + jnp.minimum(0.0, 7.0 * sine) - 0.01
    tile_f = jnp.clip(jnp.floor(lowest * (1.0 / 128.0)), 0.0, TILES - 2.0)
    base_f = center - 128.0 * tile_f
    first_row = (sub * TILES + tile_f.astype(jnp.int32)) * 8 + 4 * a_l
    for r in range(8):
        tsrc[r] = jnp.concatenate([x[r : r + 1, :] for x in (base_f, cosine, sine, sine)], axis=0)
        isrc[r] = first_row[r : r + 1, :]
    own_tables = [
        pltpu.make_async_copy(tsrc.at[0], stab.at[0], tsend.at[0]),
        pltpu.make_async_copy(isrc.at[0], itab.at[0], isend.at[0]),
    ]
    for c in own_tables:
        c.start()

    build_strip(strip)
    filter_rows(sino, strip, flat, msg)
    for c in own_tables:
        c.wait()

    pl.semaphore_wait(barrier, 28)

    jcopies = []
    tcopies = []
    mcopies = []
    for dj in (0, -1, 1):
        jj = (j - dj + 8) % 8
        base = m if dj == 0 else (jnp.where(j == 0, (m + 7) % 8, m) if dj == 1 else jnp.where(j == 7, (m + 1) % 8, m))
        for r in range(8):
            if dj == 0 and r == 0:
                continue
            slot = (dj + 1) * 8 + r
            jcopies.append(
                pltpu.make_async_remote_copy(
                    src_ref=jr.at[8], dst_ref=jr.at[slot],
                    send_sem=jsend.at[slot], recv_sem=jrecv.at[slot],
                    device_id=device(target_of(base, r), jj),
                )
            )
    for r in range(1, 8):
        tcopies.append(
            pltpu.make_async_remote_copy(
                src_ref=tsrc.at[r], dst_ref=stab.at[r],
                send_sem=tsend.at[r], recv_sem=trecv.at[r],
                device_id=device(target_of(m, r), j),
            )
        )
        tcopies.append(
            pltpu.make_async_remote_copy(
                src_ref=isrc.at[r], dst_ref=itab.at[r],
                send_sem=isend.at[r], recv_sem=irecv.at[r],
                device_id=device(target_of(m, r), j),
            )
        )
        mcopies.append(
            pltpu.make_async_remote_copy(
                src_ref=msg.at[0], dst_ref=msg.at[r],
                send_sem=msend.at[r], recv_sem=mrecv.at[r],
                device_id=device(target_of(m, r), j),
            )
        )
    for c in jcopies + tcopies + mcopies:
        c.start()

    last = lane == 127
    lane_1 = lane_f + 1.0

    def weights_of(r):
        own, before, after = jr[8 + r], jr[r], jr[16 + r]
        scale = 4.0 / math.sqrt(ANGLES)
        w0 = (1.0 + (own[1:2, :] - before[1:2, :]) * 1.5) * scale
        w1 = (1.0 + (after[0:1, :] - own[0:1, :]) * 1.5) * scale
        return jnp.broadcast_to(w0, shape), jnp.broadcast_to(w1, shape)

    def jitter_from(r, classes):
        for dj in classes:
            pltpu.make_async_copy(jr.at[0], jr.at[0], jrecv.at[(dj + 1) * 8 + r]).wait()

    def arrive(r):
        jitter_from(r, (0, -1, 1))
        pltpu.make_async_copy(stab.at[0], stab.at[0], trecv.at[r]).wait()
        pltpu.make_async_copy(itab.at[0], itab.at[0], irecv.at[r]).wait()
        pltpu.make_async_copy(msg.at[0], msg.at[0], mrecv.at[r]).wait()

    def expand(r, w0, w1):
        top = jnp.maximum(w0, w1)
        peak = msg[r, :, BINS:WIDE].astype(F32)
        unit[r] = peak * top * (1.0 / (FULL * 65536.0))
        gain = jnp.where(sub < 4, w0, w1) * FULL / (top * jnp.maximum(peak, TINY))
        base = r * (TILES * 8)

        def put(t, value, after):
            whole = jnp.round(value).astype(jnp.int32)
            half = jnp.round((after - value) * 0.5).astype(jnp.int32)
            taps[pl.ds(pl.multiple_of(base + t * 8, 8), 8), :] = whole * 65536 + half

        prev, prev_rolled = zero, zero
        for t in range(1, TILES):
            if t < TILES - 1:
                f = msg[r, :, 128 * (t - 1) : 128 * t].astype(F32) * gain
                rolled = pltpu.roll(f, 127, 1)
            else:
                f, rolled = zero, zero
            put(t - 1, prev, jnp.where(last, rolled, prev_rolled))
            prev, prev_rolled = f, rolled
        taps[pl.ds(pl.multiple_of(base + (TILES - 1) * 8, 8), 8), :] = jnp.zeros(shape, jnp.int32)

    def ramps_of(r):
        out_r = []
        for a in range(2):
            cos_a, sin_a = stab[r, 1, 32 * a], stab[r, 2, 32 * a]
            step = cos_a * (1.0 - 2e-6)
            rise = sin_a * sub_f
            edge = jnp.where(cos_a >= 0.0, 0.0, 127.0)
            out_r.append((step * lane_f + rise, step * jnp.broadcast_to(edge, shape) + rise))
        return out_r

    def picked(r, g, k, a, ramp):
        col = 32 * a + 16 * g + k
        start = stab[r, 0, col]
        row = jnp.clip(itab[r, 0, col], 0, ROWS - 12)
        v = ramp[0] + start
        cell = v.astype(jnp.int32)
        frac = v - cell.astype(F32)
        upper = ramp[1] + start >= lane_1
        pick = cell & 127
        words = []
        for s in range(4):
            low = jnp.broadcast_to(taps[pl.ds(row + s, 1), :], shape)
            high = jnp.broadcast_to(taps[pl.ds(row + (s + 8), 1), :], shape)
            words.append(lane_gather(jnp.where(upper, high, low), pick))
        return words, 2.0 * frac - 1.0 / 65536.0

    def block(r, g, ramps):
        for k in range(16):
            (x0, t0), (x1, t1) = [picked(r, g, k, a, ramps[a]) for a in range(2)]
            for s in range(4):
                both = (x0[s] + x1[s]).astype(F32)
                both = both + (x0[s] * 65536).astype(F32) * t0 + (x1[s] * 65536).astype(F32) * t1
                scale = jnp.broadcast_to(unit[r, s : s + 1, :], shape)
                acc[g, k, s] = acc[g, k, s] + scale * both

    def first_block(g, ramps):
        for k in range(16):
            for a in range(2):
                x, t = picked(0, g, k, a, ramps[a])
                for s in range(4):
                    alone[a, g, k, s] = x[s].astype(F32) + (x[s] * 65536).astype(F32) * t

    g_own, q_own = j // 4, j % 4
    g_far = 1 - g_own
    rcopies = []

    def finish(g, qs):
        for k in range(16):
            for s in range(4):
                turn[g, k, pl.ds(s, 8, stride=4), :] = acc[g, k, s]
        for q in range(4):
            for k in range(16):
                sendb[4 * g + q, :, 128 * k : 128 * k + 128] = turn[g, k, 8 * q : 8 * q + 8, :].astype(BF16)
        for q in qs:
            jj = 4 * g + q
            dj = (jj - j + 8) % 8
            c = pltpu.make_async_remote_copy(
                src_ref=sendb.at[jj], dst_ref=recvb.at[dj],
                send_sem=rsend.at[dj], recv_sem=rrecv.at[dj],
                device_id=device(m, jj),
            )
            c.start()
            rcopies.append(c)

    one = jnp.ones(shape, F32)
    expand(0, one, one)
    ramps = ramps_of(0)

    def own_angles(g, _):
        first_block(g, ramps)
        return 0

    lax.fori_loop(0, 2, own_angles, 0)
    jitter_from(0, (-1, 1))
    w0, w1 = weights_of(0)
    for g in range(2):
        for k in range(16):
            for s in range(4):
                scale = jnp.broadcast_to(unit[0, s : s + 1, :], shape)
                acc[g, k, s] = scale * (w0 * alone[0, g, k, s] + w1 * alone[1, g, k, s])

    def early(r, _):
        arrive(r)
        expand(r, *weights_of(r))
        ramps = ramps_of(r)
        for g in range(2):
            block(r, g, ramps)
        return 0

    lax.fori_loop(1, 4, early, 0)

    def unpack(r, _):
        arrive(r)
        expand(r, *weights_of(r))
        return 0

    lax.fori_loop(4, 8, unpack, 0)

    def late(g):
        def step(i, _):
            for r in (4 + 2 * i, 5 + 2 * i):
                block(r, g, ramps_of(r))
            return 0

        lax.fori_loop(0, 2, step, 0)

    late(g_far)
    finish(g_far, range(4))
    late(g_own)
    finish(g_own, [(q_own + i) % 4 for i in (1, 2, 3)])

    for dj in range(1, 8):
        pltpu.make_async_copy(recvb.at[0], recvb.at[0], rrecv.at[dj]).wait()
    for k in range(16):
        total = turn[g_own, k, pl.ds(pl.multiple_of(q_own * 8, 8), 8), :]
        for dj in range(1, 8):
            total = total + recvb[dj, :, 128 * k : 128 * k + 128].astype(F32)
        out[:, 128 * k : 128 * k + 128] = total
    for c in jcopies + tcopies + mcopies + rcopies:
        c.wait_send()


def body(sinogram, jitter, shift):
    vmem = pl.BlockSpec(memory_space=pltpu.VMEM)
    image = pl.pallas_call(
        kernel,
        out_shape=jax.ShapeDtypeStruct((8, BINS), F32),
        in_specs=[vmem] * 3,
        out_specs=vmem,
        scratch_shapes=[
            pltpu.VMEM((STRIP, 128), BF16),
            pltpu.VMEM((64, 256), F32),
            pltpu.VMEM((8, 8, WIDE), BF16),
            pltpu.VMEM((24, 2, 128), F32),
            pltpu.VMEM((ROWS, 128), jnp.int32),
            pltpu.VMEM((8, 8, 128), F32),
            pltpu.VMEM((2, 2, 16, 4, 8, 128), F32),
            pltpu.VMEM((8, 4, 128), F32),
            pltpu.VMEM((8, 1, 128), jnp.int32),
            pltpu.SMEM((8, 4, 128), F32),
            pltpu.SMEM((8, 1, 128), jnp.int32),
            pltpu.VMEM((2, 16, 4, 8, 128), F32),
            pltpu.VMEM((2, 16, 32, 128), F32),
            pltpu.VMEM((8, 8, BINS), BF16),
            pltpu.VMEM((8, 8, BINS), BF16),
            pltpu.SemaphoreType.DMA((24,)),
            pltpu.SemaphoreType.DMA((24,)),
            pltpu.SemaphoreType.DMA((8,)),
            pltpu.SemaphoreType.DMA((8,)),
            pltpu.SemaphoreType.DMA((8,)),
            pltpu.SemaphoreType.DMA((8,)),
            pltpu.SemaphoreType.DMA((8,)),
            pltpu.SemaphoreType.DMA((8,)),
            pltpu.SemaphoreType.DMA((8,)),
            pltpu.SemaphoreType.DMA((8,)),
        ],
        compiler_params=pltpu.CompilerParams(collective_id=0, has_side_effects=True),
    )(sinogram, jitter.reshape(1, 2), shift.reshape(1, 128))
    return image.reshape(2, 4, BINS)


def solution(mesh):
    return jax.shard_map(
        body,
        mesh=mesh,
        in_specs=(P("blk", "slab", None), P("blk"), P()),
        out_specs=P("blk", "slab", None),
        check_vma=False,
    )
```

```python
import functools
import math

import jax
import jax.numpy as jnp
from jax import lax
from jax.experimental import pallas as pl
from jax.experimental.pallas import tpu as pltpu
from jax.sharding import PartitionSpec as P

BINS = 2048
ANGLES = 128
NROWS = 128
TILES = 18
STRIP = 3968
ROWS = 8 * TILES * 8
WIDE = BINS + 128
FULL = 16383.0
TINY = 1e-30
F32 = jnp.float32
BF16 = jnp.bfloat16


def hop(r):
    dz = jnp.where((r == 0) | (r == 1) | (r == 2) | (r == 6), 0, 1)
    dx = jnp.where(
        (r == 0) | (r == 3), 0, jnp.where((r == 1) | (r == 4), 1, jnp.where((r == 2) | (r == 5), 3, 2))
    )
    return dz, dx


def source_of(m, r):
    dz, dx = hop(r)
    return ((m // 4 + dz) % 2) * 4 + (m % 4 + 4 - dx) % 4


def target_of(m, r):
    dz, dx = hop(r)
    return ((m // 4 + dz) % 2) * 4 + (m % 4 + dx) % 4


def lane_gather(x, idx):
    dims = lax.GatherDimensionNumbers(
        offset_dims=(),
        collapsed_slice_dims=(1,),
        start_index_map=(1,),
        operand_batching_dims=(0,),
        start_indices_batching_dims=(0,),
    )
    return lax.gather(
        x, idx[:, :, None], dims, slice_sizes=(1, 1), mode=lax.GatherScatterMode.PROMISE_IN_BOUNDS
    )


def build_strip(strip):
    shape = (128, 128)
    diff = lax.broadcasted_iota(jnp.int32, shape, 1) - lax.broadcasted_iota(jnp.int32, shape, 0)
    odd = (diff % 2) != 0
    diff_f = diff.astype(F32)

    def chunk(c, _):
        n = diff_f + (1920 - 128 * c).astype(F32)
        value = jnp.where(odd, (-1.0 / math.pi**2) / (n * n), 0.0)
        value = jnp.where(n == 0.0, 0.25, value)
        strip[pl.ds(pl.multiple_of(c * 128, 128), 128), :] = value.astype(BF16)
        return 0

    lax.fori_loop(0, STRIP // 128, chunk, 0)


def filter_rows(sino, strip, flat, msg):
    x = jnp.concatenate([sino[0].astype(F32), sino[1].astype(F32)], axis=0)
    xs = jnp.concatenate([x[:, 256 * i : 256 * i + 256] for i in range(8)], axis=0).astype(BF16)
    for d in range(-7, 8):
        rhs = jnp.concatenate(
            [strip[1920 - 128 * e : 1920 - 128 * e + 256, :] for e in (2 * d, 2 * d + 1)], axis=1
        )
        part = jnp.dot(xs, rhs, preferred_element_type=F32)
        for i in range(max(0, -d), min(8, 8 - d)):
            j = i + d
            piece = part[8 * i : 8 * i + 8, :]
            if i == 7:
                flat[8 * j : 8 * j + 8, :] = piece
            else:
                flat[8 * j : 8 * j + 8, :] += piece
    peak = jnp.zeros((8, 128), F32)
    for j in range(8):
        rows = flat[8 * j : 8 * j + 8, :].astype(BF16)
        msg[0, :, 256 * j : 256 * j + 256] = rows
        size = jnp.abs(rows.astype(F32))
        peak = jnp.maximum(peak, jnp.maximum(size[:, :128], size[:, 128:]))
    peak = jnp.broadcast_to(jnp.max(peak, axis=1, keepdims=True), (8, 128))
    peak = jnp.maximum(peak, jnp.concatenate([peak[4:8], peak[0:4]], axis=0))
    msg[0, :, BINS:WIDE] = peak.astype(BF16)


def kernel(
    sino, jit, shift, out,
    strip, flat, msg, jr, taps, unit, alone, tsrc, isrc, stab, itab, acc, turn, sendb, recvb,
    jsend, jrecv, tsend, trecv, isend, irecv, msend, mrecv, rsend, rrecv,
):
    idx = lax.axis_index("blk")
    m = idx // 8
    j = idx % 8
    barrier = pltpu.get_barrier_semaphore()
    shape = (8, 128)
    lane = lax.broadcasted_iota(jnp.int32, shape, 1)
    sub = lax.broadcasted_iota(jnp.int32, shape, 0)
    lane_f = lane.astype(F32)
    sub_f = sub.astype(F32)
    zero = jnp.zeros(shape, F32)

    def device(mm, jj):
        return {"blk": mm * 8 + jj}

    for dj in (-1, 0, 1):
        for r in range(8):
            if dj == 0 and r == 0:
                continue
            pl.semaphore_signal(barrier, inc=1, device_id=device(target_of(m, r), (j + dj + 8) % 8))
    for dj in (2, 3, 4, 5, 6):
        pl.semaphore_signal(barrier, inc=1, device_id=device(m, (j + dj) % 8))

    jv = jit[...].astype(F32)
    jr[8] = jnp.concatenate([jnp.broadcast_to(jv[:, a : a + 1], (1, 128)) for a in range(2)], axis=0)

    a_l = (lane // 32) % 2
    g_l = (lane // 16) % 2
    k_l = lane % 16
    own_jit = jnp.where(a_l == 0, jnp.broadcast_to(jv[:, 0:1], shape), jnp.broadcast_to(jv[:, 1:2], shape))
    angle = m * 16 + 2 * j + a_l
    theta = (angle.astype(F32) + own_jit) * math.pi / ANGLES
    cosine = jnp.cos(theta)
    sine = jnp.sin(theta)
    offset = lane_gather(jnp.broadcast_to(shift[...], shape), angle).astype(F32)
    center = (
        cosine * (128.0 * k_l.astype(F32) - (BINS - 1) / 2)
        + sine * ((16 * target_of(m, sub) + 8 * g_l).astype(F32) - (NROWS - 1) / 2)
        + ((BINS - 1) / 2 + 128.0 + offset)
    )
    lowest = center + jnp.minimum(0.0, 127.0 * cosine) + jnp.minimum(0.0, 7.0 * sine) - 0.01
    tile_f = jnp.clip(jnp.floor(lowest * (1.0 / 128.0)), 0.0, TILES - 2.0)
    base_f = center - 128.0 * tile_f
    first_row = (sub * TILES + tile_f.astype(jnp.int32)) * 8 + 4 * a_l
    for r in range(8):
        tsrc[r] = jnp.concatenate([x[r : r + 1, :] for x in (base_f, cosine, sine, sine)], axis=0)
        isrc[r] = first_row[r : r + 1, :]
    own_tables = [
        pltpu.make_async_copy(tsrc.at[0], stab.at[0], tsend.at[0]),
        pltpu.make_async_copy(isrc.at[0], itab.at[0], isend.at[0]),
    ]
    for c in own_tables:
        c.start()

    build_strip(strip)
    filter_rows(sino, strip, flat, msg)
    for c in own_tables:
        c.wait()

    pl.semaphore_wait(barrier, 28)

    jcopies = []
    tcopies = []
    mcopies = []
    for dj in (0, -1, 1):
        jj = (j - dj + 8) % 8
        base = m if dj == 0 else (jnp.where(j == 0, (m + 7) % 8, m) if dj == 1 else jnp.where(j == 7, (m + 1) % 8, m))
        for r in range(8):
            if dj == 0 and r == 0:
                continue
            slot = (dj + 1) * 8 + r
            jcopies.append(
                pltpu.make_async_remote_copy(
                    src_ref=jr.at[8], dst_ref=jr.at[slot],
                    send_sem=jsend.at[slot], recv_sem=jrecv.at[slot],
                    device_id=device(target_of(base, r), jj),
                )
            )
    for r in range(1, 8):
        tcopies.append(
            pltpu.make_async_remote_copy(
                src_ref=tsrc.at[r], dst_ref=stab.at[r],
                send_sem=tsend.at[r], recv_sem=trecv.at[r],
                device_id=device(target_of(m, r), j),
            )
        )
        tcopies.append(
            pltpu.make_async_remote_copy(
                src_ref=isrc.at[r], dst_ref=itab.at[r],
                send_sem=isend.at[r], recv_sem=irecv.at[r],
                device_id=device(target_of(m, r), j),
            )
        )
        mcopies.append(
            pltpu.make_async_remote_copy(
                src_ref=msg.at[0], dst_ref=msg.at[r],
                send_sem=msend.at[r], recv_sem=mrecv.at[r],
                device_id=device(target_of(m, r), j),
            )
        )
    for c in jcopies + tcopies + mcopies:
        c.start()

    last = lane == 127
    lane_1 = lane_f + 1.0

    def weights_of(r):
        own, before, after = jr[8 + r], jr[r], jr[16 + r]
        scale = 4.0 / math.sqrt(ANGLES)
        w0 = (1.0 + (own[1:2, :] - before[1:2, :]) * 1.5) * scale
        w1 = (1.0 + (after[0:1, :] - own[0:1, :]) * 1.5) * scale
        return jnp.broadcast_to(w0, shape), jnp.broadcast_to(w1, shape)

    def jitter_from(r, classes):
        for dj in classes:
            pltpu.make_async_copy(jr.at[0], jr.at[0], jrecv.at[(dj + 1) * 8 + r]).wait()

    def arrive(r):
        jitter_from(r, (0, -1, 1))
        pltpu.make_async_copy(stab.at[0], stab.at[0], trecv.at[r]).wait()
        pltpu.make_async_copy(itab.at[0], itab.at[0], irecv.at[r]).wait()
        pltpu.make_async_copy(msg.at[0], msg.at[0], mrecv.at[r]).wait()

    def expand(r, w0, w1):
        top = jnp.maximum(w0, w1)
        peak = msg[r, :, BINS:WIDE].astype(F32)
        unit[r] = peak * top * (1.0 / (FULL * 65536.0))
        gain = jnp.where(sub < 4, w0, w1) * FULL / (top * jnp.maximum(peak, TINY))
        base = r * (TILES * 8)

        def put(t, value, after):
            whole = jnp.round(value).astype(jnp.int32)
            half = jnp.round((after - value) * 0.5).astype(jnp.int32)
            taps[pl.ds(pl.multiple_of(base + t * 8, 8), 8), :] = lax.shift_left(whole, 16) + half

        prev, prev_rolled = zero, zero
        for t in range(1, TILES):
            if t < TILES - 1:
                f = msg[r, :, 128 * (t - 1) : 128 * t].astype(F32) * gain
                rolled = pltpu.roll(f, 127, 1)
            else:
                f, rolled = zero, zero
            put(t - 1, prev, jnp.where(last, rolled, prev_rolled))
            prev, prev_rolled = f, rolled
        taps[pl.ds(pl.multiple_of(base + (TILES - 1) * 8, 8), 8), :] = jnp.zeros(shape, jnp.int32)

    def ramps_of(r):
        out_r = []
        for a in range(2):
            cos_a, sin_a = stab[r, 1, 32 * a], stab[r, 2, 32 * a]
            step = cos_a * (1.0 - 2e-6)
            rise = sin_a * sub_f
            edge = jnp.where(cos_a >= 0.0, 0.0, 127.0)
            out_r.append((step * lane_f + rise, step * jnp.broadcast_to(edge, shape) + rise))
        return out_r

    def picked(r, g, k, a, ramp):
        col = 32 * a + 16 * g + k
        start = stab[r, 0, col]
        row = jnp.clip(itab[r, 0, col], 0, ROWS - 12)
        v = ramp[0] + start
        cell = v.astype(jnp.int32)
        frac = v - cell.astype(F32)
        upper = ramp[1] + start >= lane_1
        pick = cell & 127
        words = []
        for s in range(4):
            low = jnp.broadcast_to(taps[pl.ds(row + s, 1), :], shape)
            high = jnp.broadcast_to(taps[pl.ds(row + (s + 8), 1), :], shape)
            words.append(lane_gather(jnp.where(upper, high, low), pick))
        return words, 2.0 * frac - 1.0 / 65536.0

    def block(r, g, ramps):
        for k in range(16):
            (x0, t0), (x1, t1) = [picked(r, g, k, a, ramps[a]) for a in range(2)]
            for s in range(4):
                both = (x0[s] + x1[s]).astype(F32)
                both = both + lax.shift_left(x0[s], 16).astype(F32) * t0 + lax.shift_left(x1[s], 16).astype(F32) * t1
                scale = jnp.broadcast_to(unit[r, s : s + 1, :], shape)
                acc[g, k, s] = acc[g, k, s] + scale * both

    def first_block(g, ramps):
        for k in range(16):
            for a in range(2):
                x, t = picked(0, g, k, a, ramps[a])
                for s in range(4):
                    alone[a, g, k, s] = x[s].astype(F32) + lax.shift_left(x[s], 16).astype(F32) * t

    g_own, q_own = j // 4, j % 4
    g_far = 1 - g_own
    rcopies = []

    def finish(g, qs):
        for k in range(16):
            for s in range(4):
                turn[g, k, pl.ds(s, 8, stride=4), :] = acc[g, k, s]
        for q in qs:
            jj = 4 * g + q
            for k in range(16):
                rows = turn[g, k, pl.ds(pl.multiple_of(8 * q, 8), 8), :]
                sendb[jj, :, 128 * k : 128 * k + 128] = rows.astype(BF16)
            dj = (jj - j + 8) % 8
            c = pltpu.make_async_remote_copy(
                src_ref=sendb.at[jj], dst_ref=recvb.at[dj],
                send_sem=rsend.at[dj], recv_sem=rrecv.at[dj],
                device_id=device(m, jj),
            )
            c.start()
            rcopies.append(c)

    one = jnp.ones(shape, F32)
    expand(0, one, one)
    ramps = ramps_of(0)

    def own_angles(g, _):
        first_block(g, ramps)
        return 0

    lax.fori_loop(0, 2, own_angles, 0)
    jitter_from(0, (-1, 1))
    w0, w1 = weights_of(0)
    for g in range(2):
        for k in range(16):
            for s in range(4):
                scale = jnp.broadcast_to(unit[0, s : s + 1, :], shape)
                acc[g, k, s] = scale * (w0 * alone[0, g, k, s] + w1 * alone[1, g, k, s])

    def early(r, _):
        arrive(r)
        expand(r, *weights_of(r))
        ramps = ramps_of(r)
        for g in range(2):
            block(r, g, ramps)
        return 0

    lax.fori_loop(1, 4, early, 0)

    def unpack(r, _):
        arrive(r)
        expand(r, *weights_of(r))
        return 0

    lax.fori_loop(4, 8, unpack, 0)

    def late(g):
        def step(i, _):
            for r in (4 + 2 * i, 5 + 2 * i):
                block(r, g, ramps_of(r))
            return 0

        lax.fori_loop(0, 2, step, 0)

    late(g_far)
    y_odd = (j // 2) % 2
    finish(g_far, [(2 * y_odd + i) % 4 for i in range(4)])
    late(g_own)
    finish(g_own, [2 - 2 * y_odd, 3 - 2 * y_odd, 2 * y_odd + (1 - j % 2)])

    for dj in range(1, 8):
        pltpu.make_async_copy(recvb.at[0], recvb.at[0], rrecv.at[dj]).wait()
    for k in range(16):
        total = turn[g_own, k, pl.ds(pl.multiple_of(q_own * 8, 8), 8), :]
        for dj in range(1, 8):
            total = total + recvb[dj, :, 128 * k : 128 * k + 128].astype(F32)
        out[:, 128 * k : 128 * k + 128] = total
    for c in jcopies + tcopies + mcopies + rcopies:
        c.wait_send()


def body(sinogram, jitter, shift):
    vmem = pl.BlockSpec(memory_space=pltpu.VMEM)
    image = pl.pallas_call(
        kernel,
        out_shape=jax.ShapeDtypeStruct((8, BINS), F32),
        in_specs=[vmem] * 3,
        out_specs=vmem,
        scratch_shapes=[
            pltpu.VMEM((STRIP, 128), BF16),
            pltpu.VMEM((64, 256), F32),
            pltpu.VMEM((8, 8, WIDE), BF16),
            pltpu.VMEM((24, 2, 128), F32),
            pltpu.VMEM((ROWS, 128), jnp.int32),
            pltpu.VMEM((8, 8, 128), F32),
            pltpu.VMEM((2, 2, 16, 4, 8, 128), F32),
            pltpu.VMEM((8, 4, 128), F32),
            pltpu.VMEM((8, 1, 128), jnp.int32),
            pltpu.SMEM((8, 4, 128), F32),
            pltpu.SMEM((8, 1, 128), jnp.int32),
            pltpu.VMEM((2, 16, 4, 8, 128), F32),
            pltpu.VMEM((2, 16, 32, 128), F32),
            pltpu.VMEM((8, 8, BINS), BF16),
            pltpu.VMEM((8, 8, BINS), BF16),
            pltpu.SemaphoreType.DMA((24,)),
            pltpu.SemaphoreType.DMA((24,)),
            pltpu.SemaphoreType.DMA((8,)),
            pltpu.SemaphoreType.DMA((8,)),
            pltpu.SemaphoreType.DMA((8,)),
            pltpu.SemaphoreType.DMA((8,)),
            pltpu.SemaphoreType.DMA((8,)),
            pltpu.SemaphoreType.DMA((8,)),
            pltpu.SemaphoreType.DMA((8,)),
            pltpu.SemaphoreType.DMA((8,)),
        ],
        compiler_params=pltpu.CompilerParams(collective_id=0, has_side_effects=True, vmem_limit_bytes=16 * 1024 * 1024),
    )(sinogram, jitter.reshape(1, 2), shift.reshape(1, 128))
    return image.reshape(2, 4, BINS)


def solution(mesh):
    return jax.shard_map(
        body,
        mesh=mesh,
        in_specs=(P("blk", "slab", None), P("blk"), P()),
        out_specs=P("blk", "slab", None),
        check_vma=False,
    )
```

```python
import functools
import math

import jax
import jax.numpy as jnp
from jax import lax
from jax.experimental import pallas as pl
from jax.experimental.pallas import tpu as pltpu
from jax.sharding import PartitionSpec as P

BINS = 2048
ANGLES = 128
NROWS = 128
TILES = 18
STRIP = 3968
ROWS = 8 * TILES * 8
WIDE = BINS + 128
FULL = 16383.0
TINY = 1e-30
F32 = jnp.float32
BF16 = jnp.bfloat16


def hop(r):
    dz = jnp.where((r == 0) | (r == 1) | (r == 2) | (r == 6), 0, 1)
    dx = jnp.where(
        (r == 0) | (r == 3), 0, jnp.where((r == 1) | (r == 4), 1, jnp.where((r == 2) | (r == 5), 3, 2))
    )
    return dz, dx


def source_of(m, r):
    dz, dx = hop(r)
    return ((m // 4 + dz) % 2) * 4 + (m % 4 + 4 - dx) % 4


def target_of(m, r):
    dz, dx = hop(r)
    return ((m // 4 + dz) % 2) * 4 + (m % 4 + dx) % 4


def lane_gather(x, idx):
    dims = lax.GatherDimensionNumbers(
        offset_dims=(),
        collapsed_slice_dims=(1,),
        start_index_map=(1,),
        operand_batching_dims=(0,),
        start_indices_batching_dims=(0,),
    )
    return lax.gather(
        x, idx[:, :, None], dims, slice_sizes=(1, 1), mode=lax.GatherScatterMode.PROMISE_IN_BOUNDS
    )


def build_strip(strip):
    shape = (128, 128)
    diff = lax.broadcasted_iota(jnp.int32, shape, 1) - lax.broadcasted_iota(jnp.int32, shape, 0)
    odd = (diff % 2) != 0
    diff_f = diff.astype(F32)

    def chunk(c, _):
        n = diff_f + (1920 - 128 * c).astype(F32)
        value = jnp.where(odd, (-1.0 / math.pi**2) / (n * n), 0.0)
        value = jnp.where(n == 0.0, 0.25, value)
        strip[pl.ds(pl.multiple_of(c * 128, 128), 128), :] = value.astype(BF16)
        return 0

    lax.fori_loop(0, STRIP // 128, chunk, 0)


def filter_rows(sino, strip, flat, msg):
    x = jnp.concatenate([sino[0].astype(F32), sino[1].astype(F32)], axis=0)
    xs = jnp.concatenate([x[:, 256 * i : 256 * i + 256] for i in range(8)], axis=0).astype(BF16)
    for d in range(-7, 8):
        rhs = jnp.concatenate(
            [strip[1920 - 128 * e : 1920 - 128 * e + 256, :] for e in (2 * d, 2 * d + 1)], axis=1
        )
        part = jnp.dot(xs, rhs, preferred_element_type=F32)
        for i in range(max(0, -d), min(8, 8 - d)):
            j = i + d
            piece = part[8 * i : 8 * i + 8, :]
            if i == 7:
                flat[8 * j : 8 * j + 8, :] = piece
            else:
                flat[8 * j : 8 * j + 8, :] += piece
    peak = jnp.zeros((8, 128), F32)
    for j in range(8):
        rows = flat[8 * j : 8 * j + 8, :].astype(BF16)
        msg[0, :, 256 * j : 256 * j + 256] = rows
        size = jnp.abs(rows.astype(F32))
        peak = jnp.maximum(peak, jnp.maximum(size[:, :128], size[:, 128:]))
    peak = jnp.broadcast_to(jnp.max(peak, axis=1, keepdims=True), (8, 128))
    peak = jnp.maximum(peak, jnp.concatenate([peak[4:8], peak[0:4]], axis=0))
    msg[0, :, BINS:WIDE] = peak.astype(BF16)


def kernel(
    sino, jit, shift, out,
    strip, flat, msg, jr, taps, unit, alone, tsrc, isrc, stab, itab, acc, turn, sendb, recvb,
    jsend, jrecv, tsend, trecv, isend, irecv, msend, mrecv, rsend, rrecv,
):
    idx = lax.axis_index("blk")
    m = idx // 8
    j = idx % 8
    barrier = pltpu.get_barrier_semaphore()
    shape = (8, 128)
    lane = lax.broadcasted_iota(jnp.int32, shape, 1)
    sub = lax.broadcasted_iota(jnp.int32, shape, 0)
    lane_f = lane.astype(F32)
    sub_f = sub.astype(F32)
    zero = jnp.zeros(shape, F32)

    def device(mm, jj):
        return {"blk": mm * 8 + jj}

    for dj in (-1, 0, 1):
        for r in range(8):
            if dj == 0 and r == 0:
                continue
            pl.semaphore_signal(barrier, inc=1, device_id=device(target_of(m, r), (j + dj + 8) % 8))
    for dj in (2, 3, 4, 5, 6):
        pl.semaphore_signal(barrier, inc=1, device_id=device(m, (j + dj) % 8))

    jv = jit[...].astype(F32)
    jr[8] = jnp.concatenate([jnp.broadcast_to(jv[:, a : a + 1], (1, 128)) for a in range(2)], axis=0)

    a_l = (lane // 32) % 2
    g_l = (lane // 16) % 2
    k_l = lane % 16
    own_jit = jnp.where(a_l == 0, jnp.broadcast_to(jv[:, 0:1], shape), jnp.broadcast_to(jv[:, 1:2], shape))
    angle = m * 16 + 2 * j + a_l
    theta = (angle.astype(F32) + own_jit) * math.pi / ANGLES
    cosine = jnp.cos(theta)
    sine = jnp.sin(theta)
    offset = lane_gather(jnp.broadcast_to(shift[...], shape), angle).astype(F32)
    center = (
        cosine * (128.0 * k_l.astype(F32) - (BINS - 1) / 2)
        + sine * ((16 * target_of(m, sub) + 8 * g_l).astype(F32) - (NROWS - 1) / 2)
        + ((BINS - 1) / 2 + 128.0 + offset)
    )
    lowest = center + jnp.minimum(0.0, 127.0 * cosine) + jnp.minimum(0.0, 7.0 * sine) - 0.01
    tile_f = jnp.clip(jnp.floor(lowest * (1.0 / 128.0)), 0.0, TILES - 2.0)
    base_f = center - 128.0 * tile_f
    first_row = (sub * TILES + tile_f.astype(jnp.int32)) * 8 + 4 * a_l
    for r in range(8):
        tsrc[r] = jnp.concatenate([x[r : r + 1, :] for x in (base_f, cosine, sine, sine)], axis=0)
        isrc[r] = first_row[r : r + 1, :]
    own_tables = [
        pltpu.make_async_copy(tsrc.at[0], stab.at[0], tsend.at[0]),
        pltpu.make_async_copy(isrc.at[0], itab.at[0], isend.at[0]),
    ]
    for c in own_tables:
        c.start()

    build_strip(strip)
    filter_rows(sino, strip, flat, msg)
    for c in own_tables:
        c.wait()

    pl.semaphore_wait(barrier, 28)

    jcopies = []
    tcopies = []
    mcopies = []
    for dj in (0, -1, 1):
        jj = (j - dj + 8) % 8
        base = m if dj == 0 else (jnp.where(j == 0, (m + 7) % 8, m) if dj == 1 else jnp.where(j == 7, (m + 1) % 8, m))
        for r in range(8):
            if dj == 0 and r == 0:
                continue
            slot = (dj + 1) * 8 + r
            jcopies.append(
                pltpu.make_async_remote_copy(
                    src_ref=jr.at[8], dst_ref=jr.at[slot],
                    send_sem=jsend.at[slot], recv_sem=jrecv.at[slot],
                    device_id=device(target_of(base, r), jj),
                )
            )
    for r in range(1, 8):
        tcopies.append(
            pltpu.make_async_remote_copy(
                src_ref=tsrc.at[r], dst_ref=stab.at[r],
                send_sem=tsend.at[r], recv_sem=trecv.at[r],
                device_id=device(target_of(m, r), j),
            )
        )
        tcopies.append(
            pltpu.make_async_remote_copy(
                src_ref=isrc.at[r], dst_ref=itab.at[r],
                send_sem=isend.at[r], recv_sem=irecv.at[r],
                device_id=device(target_of(m, r), j),
            )
        )
        mcopies.append(
            pltpu.make_async_remote_copy(
                src_ref=msg.at[0], dst_ref=msg.at[r],
                send_sem=msend.at[r], recv_sem=mrecv.at[r],
                device_id=device(target_of(m, r), j),
            )
        )
    for c in jcopies + tcopies + mcopies:
        c.start()

    last = lane == 127
    lane_1 = lane_f + 1.0

    def weights_of(r):
        own, before, after = jr[8 + r], jr[r], jr[16 + r]
        scale = 4.0 / math.sqrt(ANGLES)
        w0 = (1.0 + (own[1:2, :] - before[1:2, :]) * 1.5) * scale
        w1 = (1.0 + (after[0:1, :] - own[0:1, :]) * 1.5) * scale
        return jnp.broadcast_to(w0, shape), jnp.broadcast_to(w1, shape)

    def jitter_from(r, classes):
        for dj in classes:
            pltpu.make_async_copy(jr.at[0], jr.at[0], jrecv.at[(dj + 1) * 8 + r]).wait()

    def arrive(r):
        jitter_from(r, (0, -1, 1))
        pltpu.make_async_copy(stab.at[0], stab.at[0], trecv.at[r]).wait()
        pltpu.make_async_copy(itab.at[0], itab.at[0], irecv.at[r]).wait()
        pltpu.make_async_copy(msg.at[0], msg.at[0], mrecv.at[r]).wait()

    def expand(r, w0, w1):
        top = jnp.maximum(w0, w1)
        peak = msg[r, :, BINS:WIDE].astype(F32)
        unit[r] = peak * top * (1.0 / (FULL * 65536.0))
        gain = jnp.where(sub < 4, w0, w1) * FULL / (top * jnp.maximum(peak, TINY))
        base = r * (TILES * 8)

        def put(t, value, after):
            whole = jnp.round(value).astype(jnp.int32)
            half = jnp.round((after - value) * 0.5).astype(jnp.int32)
            taps[pl.ds(pl.multiple_of(base + t * 8, 8), 8), :] = lax.shift_left(whole, 16) + half

        prev, prev_rolled = zero, zero
        for t in range(1, TILES):
            if t < TILES - 1:
                f = msg[r, :, 128 * (t - 1) : 128 * t].astype(F32) * gain
                rolled = pltpu.roll(f, 127, 1)
            else:
                f, rolled = zero, zero
            put(t - 1, prev, jnp.where(last, rolled, prev_rolled))
            prev, prev_rolled = f, rolled
        taps[pl.ds(pl.multiple_of(base + (TILES - 1) * 8, 8), 8), :] = jnp.zeros(shape, jnp.int32)

    def ramps_of(r):
        out_r = []
        for a in range(2):
            cos_a, sin_a = stab[r, 1, 32 * a], stab[r, 2, 32 * a]
            step = cos_a * (1.0 - 2e-6)
            rise = sin_a * sub_f
            edge = jnp.where(cos_a >= 0.0, 0.0, 127.0)
            out_r.append((step * lane_f + rise, step * jnp.broadcast_to(edge, shape) + rise))
        return out_r

    def picked(r, g, k, a, ramp):
        col = 32 * a + 16 * g + k
        start = stab[r, 0, col]
        row = jnp.clip(itab[r, 0, col], 0, ROWS - 12)
        v = ramp[0] + start
        cell = v.astype(jnp.int32)
        frac = v - cell.astype(F32)
        upper = ramp[1] + start >= lane_1
        pick = cell & 127
        words = []
        for s in range(4):
            low = jnp.broadcast_to(taps[pl.ds(row + s, 1), :], shape)
            high = jnp.broadcast_to(taps[pl.ds(row + (s + 8), 1), :], shape)
            words.append(lane_gather(jnp.where(upper, high, low), pick))
        return words, 2.0 * frac - 1.0 / 65536.0

    def source_terms(r, g, k, ramps):
        (x0, t0), (x1, t1) = [picked(r, g, k, a, ramps[a]) for a in range(2)]
        terms = []
        for s in range(4):
            both = (x0[s] + x1[s]).astype(F32)
            both = both + lax.shift_left(x0[s], 16).astype(F32) * t0 + lax.shift_left(x1[s], 16).astype(F32) * t1
            terms.append(jnp.broadcast_to(unit[r, s : s + 1, :], shape) * both)
        return terms

    def block(r, g, ramps):
        for k in range(16):
            for s, term in enumerate(source_terms(r, g, k, ramps)):
                acc[g, k, s] = acc[g, k, s] + term

    def first_block(g, ramps):
        for k in range(16):
            for a in range(2):
                x, t = picked(0, g, k, a, ramps[a])
                for s in range(4):
                    alone[a, g, k, s] = x[s].astype(F32) + lax.shift_left(x[s], 16).astype(F32) * t

    g_own, q_own = j // 4, j % 4
    g_far = 1 - g_own
    rcopies = []

    def late(g, half, qs):
        ramps = [ramps_of(r) for r in range(4, 8)]
        for k in range(8 * half, 8 * half + 8):
            total = [acc[g, k, s] for s in range(4)]
            for r in range(4, 8):
                scaled = source_terms(r, g, k, ramps[r - 4])
                total = [t + c for t, c in zip(total, scaled)]
            for s in range(4):
                turn[g, k, pl.ds(s, 8, stride=4), :] = total[s]
        columns = pl.ds(1024 * half, 1024)
        for q in qs:
            jj = 4 * g + q
            for k in range(8 * half, 8 * half + 8):
                rows = turn[g, k, pl.ds(pl.multiple_of(8 * q, 8), 8), :]
                sendb[jj, :, 128 * k : 128 * k + 128] = rows.astype(BF16)
            dj = (jj - j + 8) % 8
            c = pltpu.make_async_remote_copy(
                src_ref=sendb.at[jj, :, columns], dst_ref=recvb.at[dj, :, columns],
                send_sem=rsend.at[half, dj], recv_sem=rrecv.at[half, dj],
                device_id=device(m, jj),
            )
            c.start()
            rcopies.append(c)

    one = jnp.ones(shape, F32)
    expand(0, one, one)
    ramps = ramps_of(0)

    def own_angles(g, _):
        first_block(g, ramps)
        return 0

    lax.fori_loop(0, 2, own_angles, 0)
    jitter_from(0, (-1, 1))
    w0, w1 = weights_of(0)
    for g in range(2):
        for k in range(16):
            for s in range(4):
                scale = jnp.broadcast_to(unit[0, s : s + 1, :], shape)
                acc[g, k, s] = scale * (w0 * alone[0, g, k, s] + w1 * alone[1, g, k, s])

    def early(r, _):
        arrive(r)
        expand(r, *weights_of(r))
        ramps = ramps_of(r)
        for g in range(2):
            block(r, g, ramps)
        return 0

    lax.fori_loop(1, 4, early, 0)

    def unpack(r, _):
        arrive(r)
        expand(r, *weights_of(r))
        return 0

    lax.fori_loop(4, 8, unpack, 0)

    y_odd = (j // 2) % 2
    for half in range(2):
        late(g_far, half, [(2 * y_odd + i) % 4 for i in range(4)])
    for half in range(2):
        late(g_own, half, [2 - 2 * y_odd, 3 - 2 * y_odd, 2 * y_odd + (1 - j % 2)])

    half_row = recvb.at[0, :, pl.ds(0, 1024)]
    for k in range(16):
        if k % 8 == 0:
            for dj in range(1, 8):
                pltpu.make_async_copy(half_row, half_row, rrecv.at[k // 8, dj]).wait()
        total = turn[g_own, k, pl.ds(pl.multiple_of(q_own * 8, 8), 8), :]
        for dj in range(1, 8):
            total = total + recvb[dj, :, 128 * k : 128 * k + 128].astype(F32)
        out[:, 128 * k : 128 * k + 128] = total
    for c in jcopies + tcopies + mcopies + rcopies:
        c.wait_send()


def body(sinogram, jitter, shift):
    vmem = pl.BlockSpec(memory_space=pltpu.VMEM)
    image = pl.pallas_call(
        kernel,
        out_shape=jax.ShapeDtypeStruct((8, BINS), F32),
        in_specs=[vmem] * 3,
        out_specs=vmem,
        scratch_shapes=[
            pltpu.VMEM((STRIP, 128), BF16),
            pltpu.VMEM((64, 256), F32),
            pltpu.VMEM((8, 8, WIDE), BF16),
            pltpu.VMEM((24, 2, 128), F32),
            pltpu.VMEM((ROWS, 128), jnp.int32),
            pltpu.VMEM((8, 8, 128), F32),
            pltpu.VMEM((2, 2, 16, 4, 8, 128), F32),
            pltpu.VMEM((8, 4, 128), F32),
            pltpu.VMEM((8, 1, 128), jnp.int32),
            pltpu.SMEM((8, 4, 128), F32),
            pltpu.SMEM((8, 1, 128), jnp.int32),
            pltpu.VMEM((2, 16, 4, 8, 128), F32),
            pltpu.VMEM((2, 16, 32, 128), F32),
            pltpu.VMEM((8, 8, BINS), BF16),
            pltpu.VMEM((8, 8, BINS), BF16),
            pltpu.SemaphoreType.DMA((24,)),
            pltpu.SemaphoreType.DMA((24,)),
            pltpu.SemaphoreType.DMA((8,)),
            pltpu.SemaphoreType.DMA((8,)),
            pltpu.SemaphoreType.DMA((8,)),
            pltpu.SemaphoreType.DMA((8,)),
            pltpu.SemaphoreType.DMA((8,)),
            pltpu.SemaphoreType.DMA((8,)),
            pltpu.SemaphoreType.DMA((2, 8)),
            pltpu.SemaphoreType.DMA((2, 8)),
        ],
        compiler_params=pltpu.CompilerParams(collective_id=0, has_side_effects=True, vmem_limit_bytes=16 * 1024 * 1024),
    )(sinogram, jitter.reshape(1, 2), shift.reshape(1, 128))
    return image.reshape(2, 4, BINS)


def solution(mesh):
    return jax.shard_map(
        body,
        mesh=mesh,
        in_specs=(P("blk", "slab", None), P("blk"), P()),
        out_specs=P("blk", "slab", None),
        check_vma=False,
    )
```

```python
import functools
import math

import jax
import jax.numpy as jnp
from jax import lax
from jax.experimental import pallas as pl
from jax.experimental.pallas import tpu as pltpu
from jax.sharding import PartitionSpec as P

BINS = 2048
ANGLES = 128
NROWS = 128
TILES = 18
STRIP = 3968
ROWS = 8 * TILES * 8
WIDE = BINS + 128
FULL = 16383.0
TINY = 1e-30
F32 = jnp.float32
BF16 = jnp.bfloat16


def hop(r):
    dz = jnp.where((r == 0) | (r == 1) | (r == 2) | (r == 6), 0, 1)
    dx = jnp.where(
        (r == 0) | (r == 3), 0, jnp.where((r == 1) | (r == 4), 1, jnp.where((r == 2) | (r == 5), 3, 2))
    )
    return dz, dx


def source_of(m, r):
    dz, dx = hop(r)
    return ((m // 4 + dz) % 2) * 4 + (m % 4 + 4 - dx) % 4


def target_of(m, r):
    dz, dx = hop(r)
    return ((m // 4 + dz) % 2) * 4 + (m % 4 + dx) % 4


def lane_gather(x, idx):
    dims = lax.GatherDimensionNumbers(
        offset_dims=(),
        collapsed_slice_dims=(1,),
        start_index_map=(1,),
        operand_batching_dims=(0,),
        start_indices_batching_dims=(0,),
    )
    return lax.gather(
        x, idx[:, :, None], dims, slice_sizes=(1, 1), mode=lax.GatherScatterMode.PROMISE_IN_BOUNDS
    )


def build_strip(strip):
    shape = (128, 128)
    diff = lax.broadcasted_iota(jnp.int32, shape, 1) - lax.broadcasted_iota(jnp.int32, shape, 0)
    odd = (diff % 2) != 0
    diff_f = diff.astype(F32)

    def chunk(c, _):
        n = diff_f + (1920 - 128 * c).astype(F32)
        value = jnp.where(odd, (-1.0 / math.pi**2) / (n * n), 0.0)
        value = jnp.where(n == 0.0, 0.25, value)
        strip[pl.ds(pl.multiple_of(c * 128, 128), 128), :] = value.astype(BF16)
        return 0

    lax.fori_loop(0, STRIP // 128, chunk, 0)


def filter_rows(sino, strip, flat, msg):
    x = jnp.concatenate([sino[0].astype(F32), sino[1].astype(F32)], axis=0)
    xs = jnp.concatenate([x[:, 256 * i : 256 * i + 256] for i in range(8)], axis=0).astype(BF16)
    for d in range(-7, 8):
        rhs = jnp.concatenate(
            [strip[1920 - 128 * e : 1920 - 128 * e + 256, :] for e in (2 * d, 2 * d + 1)], axis=1
        )
        part = jnp.dot(xs, rhs, preferred_element_type=F32)
        for i in range(max(0, -d), min(8, 8 - d)):
            j = i + d
            piece = part[8 * i : 8 * i + 8, :]
            if i == 7:
                flat[8 * j : 8 * j + 8, :] = piece
            else:
                flat[8 * j : 8 * j + 8, :] += piece
    peak = jnp.zeros((8, 128), F32)
    for j in range(8):
        rows = flat[8 * j : 8 * j + 8, :].astype(BF16)
        msg[0, :, 256 * j : 256 * j + 256] = rows
        size = jnp.abs(rows.astype(F32))
        peak = jnp.maximum(peak, jnp.maximum(size[:, :128], size[:, 128:]))
    peak = jnp.broadcast_to(jnp.max(peak, axis=1, keepdims=True), (8, 128))
    peak = jnp.maximum(peak, jnp.concatenate([peak[4:8], peak[0:4]], axis=0))
    msg[0, :, BINS:WIDE] = peak.astype(BF16)


def kernel(
    sino, jit, shift, out,
    strip, flat, msg, jr, taps, unit, alone, tsrc, isrc, stab, itab, acc, turn, sendb, recvb,
    jsend, jrecv, tsend, trecv, isend, irecv, msend, mrecv, rsend, rrecv,
):
    idx = lax.axis_index("blk")
    m = idx // 8
    j = idx % 8
    barrier = pltpu.get_barrier_semaphore()
    shape = (8, 128)
    lane = lax.broadcasted_iota(jnp.int32, shape, 1)
    sub = lax.broadcasted_iota(jnp.int32, shape, 0)
    lane_f = lane.astype(F32)
    sub_f = sub.astype(F32)
    zero = jnp.zeros(shape, F32)

    def device(mm, jj):
        return {"blk": mm * 8 + jj}

    for dj in (-1, 0, 1):
        for r in range(8):
            if dj == 0 and r == 0:
                continue
            pl.semaphore_signal(barrier, inc=1, device_id=device(target_of(m, r), (j + dj + 8) % 8))
    for dj in (2, 3, 4, 5, 6):
        pl.semaphore_signal(barrier, inc=1, device_id=device(m, (j + dj) % 8))

    jv = jit[...].astype(F32)
    jr[8] = jnp.concatenate([jnp.broadcast_to(jv[:, a : a + 1], (1, 128)) for a in range(2)], axis=0)

    a_l = (lane // 32) % 2
    g_l = (lane // 16) % 2
    k_l = lane % 16
    own_jit = jnp.where(a_l == 0, jnp.broadcast_to(jv[:, 0:1], shape), jnp.broadcast_to(jv[:, 1:2], shape))
    angle = m * 16 + 2 * j + a_l
    theta = (angle.astype(F32) + own_jit) * math.pi / ANGLES
    cosine = jnp.cos(theta)
    sine = jnp.sin(theta)
    offset = lane_gather(jnp.broadcast_to(shift[...], shape), angle).astype(F32)
    center = (
        cosine * (128.0 * k_l.astype(F32) - (BINS - 1) / 2)
        + sine * ((16 * target_of(m, sub) + 8 * g_l).astype(F32) - (NROWS - 1) / 2)
        + ((BINS - 1) / 2 + 128.0 + offset)
    )
    lowest = center + jnp.minimum(0.0, 127.0 * cosine) + jnp.minimum(0.0, 7.0 * sine) - 0.01
    tile_f = jnp.clip(jnp.floor(lowest * (1.0 / 128.0)), 0.0, TILES - 2.0)
    base_f = center - 128.0 * tile_f
    first_row = (sub * TILES + tile_f.astype(jnp.int32)) * 8 + 4 * a_l
    for r in range(8):
        tsrc[r] = jnp.concatenate([x[r : r + 1, :] for x in (base_f, cosine, sine, sine)], axis=0)
        isrc[r] = first_row[r : r + 1, :]
    own_tables = [
        pltpu.make_async_copy(tsrc.at[0], stab.at[0], tsend.at[0]),
        pltpu.make_async_copy(isrc.at[0], itab.at[0], isend.at[0]),
    ]
    for c in own_tables:
        c.start()

    build_strip(strip)
    filter_rows(sino, strip, flat, msg)
    for c in own_tables:
        c.wait()

    pl.semaphore_wait(barrier, 28)

    jcopies = []
    tcopies = []
    mcopies = []
    for dj in (0, -1, 1):
        jj = (j - dj + 8) % 8
        base = m if dj == 0 else (jnp.where(j == 0, (m + 7) % 8, m) if dj == 1 else jnp.where(j == 7, (m + 1) % 8, m))
        for r in range(8):
            if dj == 0 and r == 0:
                continue
            slot = (dj + 1) * 8 + r
            jcopies.append(
                pltpu.make_async_remote_copy(
                    src_ref=jr.at[8], dst_ref=jr.at[slot],
                    send_sem=jsend.at[slot], recv_sem=jrecv.at[slot],
                    device_id=device(target_of(base, r), jj),
                )
            )
    for r in range(1, 8):
        tcopies.append(
            pltpu.make_async_remote_copy(
                src_ref=tsrc.at[r], dst_ref=stab.at[r],
                send_sem=tsend.at[r], recv_sem=trecv.at[r],
                device_id=device(target_of(m, r), j),
            )
        )
        tcopies.append(
            pltpu.make_async_remote_copy(
                src_ref=isrc.at[r], dst_ref=itab.at[r],
                send_sem=isend.at[r], recv_sem=irecv.at[r],
                device_id=device(target_of(m, r), j),
            )
        )
        mcopies.append(
            pltpu.make_async_remote_copy(
                src_ref=msg.at[0], dst_ref=msg.at[r],
                send_sem=msend.at[r], recv_sem=mrecv.at[r],
                device_id=device(target_of(m, r), j),
            )
        )
    for c in jcopies + tcopies + mcopies:
        c.start()

    last = lane == 127
    lane_1 = lane_f + 1.0

    def weights_of(r):
        own, before, after = jr[8 + r], jr[r], jr[16 + r]
        scale = 4.0 / math.sqrt(ANGLES)
        w0 = (1.0 + (own[1:2, :] - before[1:2, :]) * 1.5) * scale
        w1 = (1.0 + (after[0:1, :] - own[0:1, :]) * 1.5) * scale
        return jnp.broadcast_to(w0, shape), jnp.broadcast_to(w1, shape)

    def jitter_from(r, classes):
        for dj in classes:
            pltpu.make_async_copy(jr.at[0], jr.at[0], jrecv.at[(dj + 1) * 8 + r]).wait()

    def arrive(r):
        jitter_from(r, (0, -1, 1))
        pltpu.make_async_copy(stab.at[0], stab.at[0], trecv.at[r]).wait()
        pltpu.make_async_copy(itab.at[0], itab.at[0], irecv.at[r]).wait()
        pltpu.make_async_copy(msg.at[0], msg.at[0], mrecv.at[r]).wait()

    def expand(r, w0, w1):
        top = jnp.maximum(w0, w1)
        peak = msg[r, :, BINS:WIDE].astype(F32)
        unit[r] = peak * top * (1.0 / (FULL * 65536.0))
        gain = jnp.where(sub < 4, w0, w1) * FULL / (top * jnp.maximum(peak, TINY))
        base = r * (TILES * 8)

        def put(t, value, after):
            whole = jnp.round(value).astype(jnp.int32)
            half = jnp.round((after - value) * 0.5).astype(jnp.int32)
            taps[pl.ds(pl.multiple_of(base + t * 8, 8), 8), :] = lax.shift_left(whole, 16) + half

        prev, prev_rolled = zero, zero
        for t in range(1, TILES):
            if t < TILES - 1:
                f = msg[r, :, 128 * (t - 1) : 128 * t].astype(F32) * gain
                rolled = pltpu.roll(f, 127, 1)
            else:
                f, rolled = zero, zero
            put(t - 1, prev, jnp.where(last, rolled, prev_rolled))
            prev, prev_rolled = f, rolled
        taps[pl.ds(pl.multiple_of(base + (TILES - 1) * 8, 8), 8), :] = jnp.zeros(shape, jnp.int32)

    def ramps_of(r):
        out_r = []
        for a in range(2):
            cos_a, sin_a = stab[r, 1, 32 * a], stab[r, 2, 32 * a]
            step = cos_a * (1.0 - 2e-6)
            rise = sin_a * sub_f
            edge = jnp.where(cos_a >= 0.0, 0.0, 127.0)
            out_r.append((step * lane_f + rise, step * jnp.broadcast_to(edge, shape) + rise))
        return out_r

    def picked(r, g, k, a, ramp):
        col = 32 * a + 16 * g + k
        start = stab[r, 0, col]
        row = jnp.clip(itab[r, 0, col], 0, ROWS - 12)
        v = ramp[0] + start
        cell = v.astype(jnp.int32)
        frac = v - cell.astype(F32)
        upper = ramp[1] + start >= lane_1
        pick = cell & 127
        words = []
        for s in range(4):
            low = jnp.broadcast_to(taps[pl.ds(row + s, 1), :], shape)
            high = jnp.broadcast_to(taps[pl.ds(row + (s + 8), 1), :], shape)
            words.append(lane_gather(jnp.where(upper, high, low), pick))
        return words, 2.0 * frac - 1.0 / 65536.0

    def source_terms(r, g, k, ramps):
        (x0, t0), (x1, t1) = [picked(r, g, k, a, ramps[a]) for a in range(2)]
        terms = []
        for s in range(4):
            both = (x0[s] + x1[s]).astype(F32)
            both = both + lax.shift_left(x0[s], 16).astype(F32) * t0 + lax.shift_left(x1[s], 16).astype(F32) * t1
            terms.append(jnp.broadcast_to(unit[r, s : s + 1, :], shape) * both)
        return terms

    def block(r, g, ramps):
        for k in range(16):
            for s, term in enumerate(source_terms(r, g, k, ramps)):
                acc[g, k, s] = acc[g, k, s] + term

    def first_block(g, ramps):
        for k in range(16):
            for a in range(2):
                x, t = picked(0, g, k, a, ramps[a])
                for s in range(4):
                    alone[a, g, k, s] = x[s].astype(F32) + lax.shift_left(x[s], 16).astype(F32) * t

    g_own, q_own = j // 4, j % 4
    g_far = 1 - g_own
    rcopies = []

    def late(g, half, qs):
        ramps = [ramps_of(r) for r in range(4, 8)]
        for k in range(8 * half, 8 * half + 8):
            total = [acc[g, k, s] for s in range(4)]
            for r in range(4, 8):
                scaled = source_terms(r, g, k, ramps[r - 4])
                total = [t + c for t, c in zip(total, scaled)]
            for s in range(4):
                turn[g, k, pl.ds(s, 8, stride=4), :] = total[s]
        columns = pl.ds(1024 * half, 1024)
        for q in qs:
            jj = 4 * g + q
            for k in range(8 * half, 8 * half + 8):
                rows = turn[g, k, pl.ds(pl.multiple_of(8 * q, 8), 8), :]
                sendb[jj, :, 128 * k : 128 * k + 128] = rows.astype(BF16)
            dj = (jj - j + 8) % 8
            c = pltpu.make_async_remote_copy(
                src_ref=sendb.at[jj, :, columns], dst_ref=recvb.at[dj, :, columns],
                send_sem=rsend.at[half, dj], recv_sem=rrecv.at[half, dj],
                device_id=device(m, jj),
            )
            c.start()
            rcopies.append(c)

    one = jnp.ones(shape, F32)
    expand(0, one, one)
    ramps = ramps_of(0)

    def own_angles(g, _):
        first_block(g, ramps)
        return 0

    lax.fori_loop(0, 2, own_angles, 0)
    jitter_from(0, (-1, 1))
    w0, w1 = weights_of(0)
    for g in range(2):
        for k in range(16):
            for s in range(4):
                scale = jnp.broadcast_to(unit[0, s : s + 1, :], shape)
                acc[g, k, s] = scale * (w0 * alone[0, g, k, s] + w1 * alone[1, g, k, s])

    def early(r, _):
        arrive(r)
        expand(r, *weights_of(r))
        ramps = ramps_of(r)
        for g in range(2):
            block(r, g, ramps)
        return 0

    lax.fori_loop(1, 4, early, 0)

    for r in range(4, 8):
        arrive(r)
    for r in range(4, 8):
        expand(r, *weights_of(r))

    y_odd = (j // 2) % 2
    for half in range(2):
        late(g_far, half, [(2 * y_odd + i) % 4 for i in range(4)])
    for half in range(2):
        late(g_own, half, [2 - 2 * y_odd, 3 - 2 * y_odd, 2 * y_odd + (1 - j % 2)])

    half_row = recvb.at[0, :, pl.ds(0, 1024)]
    for k in range(16):
        if k % 8 == 0:
            for dj in range(1, 8):
                pltpu.make_async_copy(half_row, half_row, rrecv.at[k // 8, dj]).wait()
        total = turn[g_own, k, pl.ds(pl.multiple_of(q_own * 8, 8), 8), :]
        for dj in range(1, 8):
            total = total + recvb[dj, :, 128 * k : 128 * k + 128].astype(F32)
        out[:, 128 * k : 128 * k + 128] = total
    for c in jcopies + tcopies + mcopies + rcopies:
        c.wait_send()


def body(sinogram, jitter, shift):
    vmem = pl.BlockSpec(memory_space=pltpu.VMEM)
    image = pl.pallas_call(
        kernel,
        out_shape=jax.ShapeDtypeStruct((8, BINS), F32),
        in_specs=[vmem] * 3,
        out_specs=vmem,
        scratch_shapes=[
            pltpu.VMEM((STRIP, 128), BF16),
            pltpu.VMEM((64, 256), F32),
            pltpu.VMEM((8, 8, WIDE), BF16),
            pltpu.VMEM((24, 2, 128), F32),
            pltpu.VMEM((ROWS, 128), jnp.int32),
            pltpu.VMEM((8, 8, 128), F32),
            pltpu.VMEM((2, 2, 16, 4, 8, 128), F32),
            pltpu.VMEM((8, 4, 128), F32),
            pltpu.VMEM((8, 1, 128), jnp.int32),
            pltpu.SMEM((8, 4, 128), F32),
            pltpu.SMEM((8, 1, 128), jnp.int32),
            pltpu.VMEM((2, 16, 4, 8, 128), F32),
            pltpu.VMEM((2, 16, 32, 128), F32),
            pltpu.VMEM((8, 8, BINS), BF16),
            pltpu.VMEM((8, 8, BINS), BF16),
            pltpu.SemaphoreType.DMA((24,)),
            pltpu.SemaphoreType.DMA((24,)),
            pltpu.SemaphoreType.DMA((8,)),
            pltpu.SemaphoreType.DMA((8,)),
            pltpu.SemaphoreType.DMA((8,)),
            pltpu.SemaphoreType.DMA((8,)),
            pltpu.SemaphoreType.DMA((8,)),
            pltpu.SemaphoreType.DMA((8,)),
            pltpu.SemaphoreType.DMA((2, 8)),
            pltpu.SemaphoreType.DMA((2, 8)),
        ],
        compiler_params=pltpu.CompilerParams(collective_id=0, has_side_effects=True, vmem_limit_bytes=16 * 1024 * 1024),
    )(sinogram, jitter.reshape(1, 2), shift.reshape(1, 128))
    return image.reshape(2, 4, BINS)


def solution(mesh):
    return jax.shard_map(
        body,
        mesh=mesh,
        in_specs=(P("blk", "slab", None), P("blk"), P()),
        out_specs=P("blk", "slab", None),
        check_vma=False,
    )
```

```python
import functools
import math

import jax
import jax.numpy as jnp
from jax import lax
from jax.experimental import pallas as pl
from jax.experimental.pallas import tpu as pltpu
from jax.sharding import PartitionSpec as P

BINS = 2048
ANGLES = 128
NROWS = 128
TILES = 18
STRIP = 3968
ROWS = 8 * TILES * 8
WIDE = BINS + 128
FULL = 16383.0
TINY = 1e-30
F32 = jnp.float32
BF16 = jnp.bfloat16


def hop(r):
    dz = jnp.where((r == 0) | (r == 1) | (r == 2) | (r == 6), 0, 1)
    dx = jnp.where(
        (r == 0) | (r == 3), 0, jnp.where((r == 1) | (r == 4), 1, jnp.where((r == 2) | (r == 5), 3, 2))
    )
    return dz, dx


def source_of(m, r):
    dz, dx = hop(r)
    return ((m // 4 + dz) % 2) * 4 + (m % 4 + 4 - dx) % 4


def target_of(m, r):
    dz, dx = hop(r)
    return ((m // 4 + dz) % 2) * 4 + (m % 4 + dx) % 4


def lane_gather(x, idx):
    dims = lax.GatherDimensionNumbers(
        offset_dims=(),
        collapsed_slice_dims=(1,),
        start_index_map=(1,),
        operand_batching_dims=(0,),
        start_indices_batching_dims=(0,),
    )
    return lax.gather(
        x, idx[:, :, None], dims, slice_sizes=(1, 1), mode=lax.GatherScatterMode.PROMISE_IN_BOUNDS
    )


def build_strip(strip):
    shape = (128, 128)
    diff = lax.broadcasted_iota(jnp.int32, shape, 1) - lax.broadcasted_iota(jnp.int32, shape, 0)
    odd = (diff % 2) != 0
    diff_f = diff.astype(F32)

    def chunk(c, _):
        n = diff_f + (1920 - 128 * c).astype(F32)
        value = jnp.where(odd, (-1.0 / math.pi**2) / (n * n), 0.0)
        value = jnp.where(n == 0.0, 0.25, value)
        strip[pl.ds(pl.multiple_of(c * 128, 128), 128), :] = value.astype(BF16)
        return 0

    lax.fori_loop(0, STRIP // 128, chunk, 0)


def filter_rows(sino, strip, flat, msg):
    x = jnp.concatenate([sino[0].astype(F32), sino[1].astype(F32)], axis=0)
    xs = jnp.concatenate([x[:, 256 * i : 256 * i + 256] for i in range(8)], axis=0).astype(BF16)
    for d in range(-7, 8):
        rhs = jnp.concatenate(
            [strip[1920 - 128 * e : 1920 - 128 * e + 256, :] for e in (2 * d, 2 * d + 1)], axis=1
        )
        part = jnp.dot(xs, rhs, preferred_element_type=F32)
        for i in range(max(0, -d), min(8, 8 - d)):
            j = i + d
            piece = part[8 * i : 8 * i + 8, :]
            if i == 7:
                flat[8 * j : 8 * j + 8, :] = piece
            else:
                flat[8 * j : 8 * j + 8, :] += piece
    peak = jnp.zeros((8, 128), F32)
    for j in range(8):
        rows = flat[8 * j : 8 * j + 8, :].astype(BF16)
        msg[0, :, 256 * j : 256 * j + 256] = rows
        size = jnp.abs(rows.astype(F32))
        peak = jnp.maximum(peak, jnp.maximum(size[:, :128], size[:, 128:]))
    peak = jnp.broadcast_to(jnp.max(peak, axis=1, keepdims=True), (8, 128))
    peak = jnp.maximum(peak, jnp.concatenate([peak[4:8], peak[0:4]], axis=0))
    msg[0, :, BINS:WIDE] = peak.astype(BF16)


def kernel(
    sino, jit, shift, out,
    strip, flat, msg, jr, taps, unit, alone, tsrc, isrc, stab, itab, acc, turn, sendb, recvb,
    jsend, jrecv, tsend, trecv, isend, irecv, msend, mrecv, rsend, rrecv,
):
    idx = lax.axis_index("blk")
    m = idx // 8
    j = idx % 8
    barrier = pltpu.get_barrier_semaphore()
    shape = (8, 128)
    lane = lax.broadcasted_iota(jnp.int32, shape, 1)
    sub = lax.broadcasted_iota(jnp.int32, shape, 0)
    lane_f = lane.astype(F32)
    sub_f = sub.astype(F32)
    zero = jnp.zeros(shape, F32)

    def device(mm, jj):
        return {"blk": mm * 8 + jj}

    for dj in (-1, 0, 1):
        for r in range(8):
            if dj == 0 and r == 0:
                continue
            pl.semaphore_signal(barrier, inc=1, device_id=device(target_of(m, r), (j + dj + 8) % 8))
    for dj in (2, 3, 4, 5, 6):
        pl.semaphore_signal(barrier, inc=1, device_id=device(m, (j + dj) % 8))

    jv = jit[...].astype(F32)
    jr[8] = jnp.concatenate([jnp.broadcast_to(jv[:, a : a + 1], (1, 128)) for a in range(2)], axis=0)

    a_l = (lane // 32) % 2
    g_l = (lane // 16) % 2
    k_l = lane % 16
    own_jit = jnp.where(a_l == 0, jnp.broadcast_to(jv[:, 0:1], shape), jnp.broadcast_to(jv[:, 1:2], shape))
    angle = m * 16 + 2 * j + a_l
    theta = (angle.astype(F32) + own_jit) * math.pi / ANGLES
    cosine = jnp.cos(theta)
    sine = jnp.sin(theta)
    offset = lane_gather(jnp.broadcast_to(shift[...], shape), angle).astype(F32)
    center = (
        cosine * (128.0 * k_l.astype(F32) - (BINS - 1) / 2)
        + sine * ((16 * target_of(m, sub) + 8 * g_l).astype(F32) - (NROWS - 1) / 2)
        + ((BINS - 1) / 2 + 128.0 + offset)
    )
    lowest = center + jnp.minimum(0.0, 127.0 * cosine) + jnp.minimum(0.0, 7.0 * sine) - 0.01
    tile_f = jnp.clip(jnp.floor(lowest * (1.0 / 128.0)), 0.0, TILES - 2.0)
    base_f = center - 128.0 * tile_f
    first_row = (sub * TILES + tile_f.astype(jnp.int32)) * 8 + 4 * a_l
    for r in range(8):
        tsrc[r] = jnp.concatenate([x[r : r + 1, :] for x in (base_f, cosine, sine, sine)], axis=0)
        isrc[r] = first_row[r : r + 1, :]
    own_tables = [
        pltpu.make_async_copy(tsrc.at[0], stab.at[0], tsend.at[0]),
        pltpu.make_async_copy(isrc.at[0], itab.at[0], isend.at[0]),
    ]
    for c in own_tables:
        c.start()

    build_strip(strip)
    filter_rows(sino, strip, flat, msg)
    for c in own_tables:
        c.wait()

    pl.semaphore_wait(barrier, 28)

    jcopies = []
    tcopies = []
    mcopies = []
    for dj in (0, -1, 1):
        jj = (j - dj + 8) % 8
        base = m if dj == 0 else (jnp.where(j == 0, (m + 7) % 8, m) if dj == 1 else jnp.where(j == 7, (m + 1) % 8, m))
        for r in range(8):
            if dj == 0 and r == 0:
                continue
            slot = (dj + 1) * 8 + r
            jcopies.append(
                pltpu.make_async_remote_copy(
                    src_ref=jr.at[8], dst_ref=jr.at[slot],
                    send_sem=jsend.at[slot], recv_sem=jrecv.at[slot],
                    device_id=device(target_of(base, r), jj),
                )
            )
    for r in range(1, 8):
        tcopies.append(
            pltpu.make_async_remote_copy(
                src_ref=tsrc.at[r], dst_ref=stab.at[r],
                send_sem=tsend.at[r], recv_sem=trecv.at[r],
                device_id=device(target_of(m, r), j),
            )
        )
        tcopies.append(
            pltpu.make_async_remote_copy(
                src_ref=isrc.at[r], dst_ref=itab.at[r],
                send_sem=isend.at[r], recv_sem=irecv.at[r],
                device_id=device(target_of(m, r), j),
            )
        )
        mcopies.append(
            pltpu.make_async_remote_copy(
                src_ref=msg.at[0], dst_ref=msg.at[r],
                send_sem=msend.at[r], recv_sem=mrecv.at[r],
                device_id=device(target_of(m, r), j),
            )
        )
    for c in jcopies + tcopies + mcopies:
        c.start()

    last = lane == 127
    lane_1 = lane_f + 1.0

    def weights_of(r):
        own, before, after = jr[8 + r], jr[r], jr[16 + r]
        scale = 4.0 / math.sqrt(ANGLES)
        w0 = (1.0 + (own[1:2, :] - before[1:2, :]) * 1.5) * scale
        w1 = (1.0 + (after[0:1, :] - own[0:1, :]) * 1.5) * scale
        return jnp.broadcast_to(w0, shape), jnp.broadcast_to(w1, shape)

    def jitter_from(r, classes):
        for dj in classes:
            pltpu.make_async_copy(jr.at[0], jr.at[0], jrecv.at[(dj + 1) * 8 + r]).wait()

    def arrive(r):
        jitter_from(r, (0, -1, 1))
        pltpu.make_async_copy(stab.at[0], stab.at[0], trecv.at[r]).wait()
        pltpu.make_async_copy(itab.at[0], itab.at[0], irecv.at[r]).wait()
        pltpu.make_async_copy(msg.at[0], msg.at[0], mrecv.at[r]).wait()

    def expand(r, w0, w1):
        top = jnp.maximum(w0, w1)
        peak = msg[r, :, BINS:WIDE].astype(F32)
        unit[r] = peak * top * (1.0 / (FULL * 65536.0))
        gain = jnp.where(sub < 4, w0, w1) * FULL / (top * jnp.maximum(peak, TINY))
        base = r * (TILES * 8)

        def put(t, value, after):
            whole = jnp.round(value).astype(jnp.int32)
            half = jnp.round((after - value) * 0.5).astype(jnp.int32)
            taps[pl.ds(pl.multiple_of(base + t * 8, 8), 8), :] = lax.shift_left(whole, 16) + half

        prev, prev_rolled = zero, zero
        for t in range(1, TILES):
            if t < TILES - 1:
                f = msg[r, :, 128 * (t - 1) : 128 * t].astype(F32) * gain
                rolled = pltpu.roll(f, 127, 1)
            else:
                f, rolled = zero, zero
            put(t - 1, prev, jnp.where(last, rolled, prev_rolled))
            prev, prev_rolled = f, rolled
        taps[pl.ds(pl.multiple_of(base + (TILES - 1) * 8, 8), 8), :] = jnp.zeros(shape, jnp.int32)

    def ramps_of(r):
        out_r = []
        for a in range(2):
            cos_a, sin_a = stab[r, 1, 32 * a], stab[r, 2, 32 * a]
            step = cos_a * (1.0 - 2e-6)
            rise = sin_a * sub_f
            edge = jnp.where(cos_a >= 0.0, 0.0, 127.0)
            out_r.append((step * lane_f + rise, step * jnp.broadcast_to(edge, shape) + rise))
        return out_r

    def picked(r, g, k, a, ramp):
        col = 32 * a + 16 * g + k
        start = stab[r, 0, col]
        row = jnp.clip(itab[r, 0, col], 0, ROWS - 12)
        v = ramp[0] + start
        cell = v.astype(jnp.int32)
        frac = v - cell.astype(F32)
        upper = ramp[1] + start >= lane_1
        pick = cell & 127
        words = []
        for s in range(4):
            low = jnp.broadcast_to(taps[pl.ds(row + s, 1), :], shape)
            high = jnp.broadcast_to(taps[pl.ds(row + (s + 8), 1), :], shape)
            words.append(lane_gather(jnp.where(upper, high, low), pick))
        return words, 2.0 * frac - 1.0 / 65536.0

    def source_terms(r, g, k, ramps):
        (x0, t0), (x1, t1) = [picked(r, g, k, a, ramps[a]) for a in range(2)]
        terms = []
        for s in range(4):
            both = (x0[s] + x1[s]).astype(F32)
            both = both + lax.shift_left(x0[s], 16).astype(F32) * t0 + lax.shift_left(x1[s], 16).astype(F32) * t1
            terms.append(jnp.broadcast_to(unit[r, s : s + 1, :], shape) * both)
        return terms

    def block(r, g, ramps):
        for k in range(16):
            for s, term in enumerate(source_terms(r, g, k, ramps)):
                acc[g, k, s] = acc[g, k, s] + term

    def first_block(g, ramps):
        for k in range(16):
            for a in range(2):
                x, t = picked(0, g, k, a, ramps[a])
                for s in range(4):
                    alone[a, g, k, s] = x[s].astype(F32) + lax.shift_left(x[s], 16).astype(F32) * t

    g_own, q_own = j // 4, j % 4
    g_far = 1 - g_own
    rcopies = []

    def late(g, half, qs):
        ramps = [ramps_of(r) for r in range(4, 8)]
        for k in range(8 * half, 8 * half + 8):
            total = [acc[g, k, s] for s in range(4)]
            for r in range(4, 8):
                scaled = source_terms(r, g, k, ramps[r - 4])
                total = [t + c for t, c in zip(total, scaled)]
            for s in range(4):
                turn[g, k, pl.ds(s, 8, stride=4), :] = total[s]
        columns = pl.ds(1024 * half, 1024)
        for q in qs:
            jj = 4 * g + q
            for k in range(8 * half, 8 * half + 8):
                rows = turn[g, k, pl.ds(pl.multiple_of(8 * q, 8), 8), :]
                sendb[jj, :, 128 * k : 128 * k + 128] = rows.astype(BF16)
            dj = (jj - j + 8) % 8
            c = pltpu.make_async_remote_copy(
                src_ref=sendb.at[jj, :, columns], dst_ref=recvb.at[dj, :, columns],
                send_sem=rsend.at[half, dj], recv_sem=rrecv.at[half, dj],
                device_id=device(m, jj),
            )
            c.start()
            rcopies.append(c)

    one = jnp.ones(shape, F32)
    expand(0, one, one)
    ramps = ramps_of(0)

    def own_angles(g, _):
        first_block(g, ramps)
        return 0

    lax.fori_loop(0, 2, own_angles, 0)
    jitter_from(0, (-1, 1))
    w0, w1 = weights_of(0)
    for g in range(2):
        for k in range(16):
            for s in range(4):
                scale = jnp.broadcast_to(unit[0, s : s + 1, :], shape)
                acc[g, k, s] = scale * (w0 * alone[0, g, k, s] + w1 * alone[1, g, k, s])

    def early(r, _):
        arrive(r)
        expand(r, *weights_of(r))
        ramps = ramps_of(r)
        for g in range(2):
            block(r, g, ramps)
        return 0

    early(1, 0)
    for r in (2, 3):
        arrive(r)
    for r in (2, 3):
        expand(r, *weights_of(r))
    pair_ramps = [ramps_of(r) for r in (2, 3)]

    def pair(g, _):
        for k in range(16):
            first = source_terms(2, g, k, pair_ramps[0])
            second = source_terms(3, g, k, pair_ramps[1])
            for s in range(4):
                acc[g, k, s] = acc[g, k, s] + (first[s] + second[s])
        return 0

    lax.fori_loop(0, 2, pair, 0)

    for r in range(4, 8):
        arrive(r)
    for r in range(4, 8):
        expand(r, *weights_of(r))

    y_odd = (j // 2) % 2
    for half in range(2):
        late(g_far, half, [(2 * y_odd + i) % 4 for i in range(4)])
    for half in range(2):
        late(g_own, half, [2 - 2 * y_odd, 3 - 2 * y_odd, 2 * y_odd + (1 - j % 2)])

    half_row = recvb.at[0, :, pl.ds(0, 1024)]
    for k in range(16):
        if k % 8 == 0:
            for dj in range(1, 8):
                pltpu.make_async_copy(half_row, half_row, rrecv.at[k // 8, dj]).wait()
        total = turn[g_own, k, pl.ds(pl.multiple_of(q_own * 8, 8), 8), :]
        for dj in range(1, 8):
            total = total + recvb[dj, :, 128 * k : 128 * k + 128].astype(F32)
        out[:, 128 * k : 128 * k + 128] = total
    for c in jcopies + tcopies + mcopies + rcopies:
        c.wait_send()


def body(sinogram, jitter, shift):
    vmem = pl.BlockSpec(memory_space=pltpu.VMEM)
    image = pl.pallas_call(
        kernel,
        out_shape=jax.ShapeDtypeStruct((8, BINS), F32),
        in_specs=[vmem] * 3,
        out_specs=vmem,
        scratch_shapes=[
            pltpu.VMEM((STRIP, 128), BF16),
            pltpu.VMEM((64, 256), F32),
            pltpu.VMEM((8, 8, WIDE), BF16),
            pltpu.VMEM((24, 2, 128), F32),
            pltpu.VMEM((ROWS, 128), jnp.int32),
            pltpu.VMEM((8, 8, 128), F32),
            pltpu.VMEM((2, 2, 16, 4, 8, 128), F32),
            pltpu.VMEM((8, 4, 128), F32),
            pltpu.VMEM((8, 1, 128), jnp.int32),
            pltpu.SMEM((8, 4, 128), F32),
            pltpu.SMEM((8, 1, 128), jnp.int32),
            pltpu.VMEM((2, 16, 4, 8, 128), F32),
            pltpu.VMEM((2, 16, 32, 128), F32),
            pltpu.VMEM((8, 8, BINS), BF16),
            pltpu.VMEM((8, 8, BINS), BF16),
            pltpu.SemaphoreType.DMA((24,)),
            pltpu.SemaphoreType.DMA((24,)),
            pltpu.SemaphoreType.DMA((8,)),
            pltpu.SemaphoreType.DMA((8,)),
            pltpu.SemaphoreType.DMA((8,)),
            pltpu.SemaphoreType.DMA((8,)),
            pltpu.SemaphoreType.DMA((8,)),
            pltpu.SemaphoreType.DMA((8,)),
            pltpu.SemaphoreType.DMA((2, 8)),
            pltpu.SemaphoreType.DMA((2, 8)),
        ],
        compiler_params=pltpu.CompilerParams(collective_id=0, has_side_effects=True, vmem_limit_bytes=16 * 1024 * 1024),
    )(sinogram, jitter.reshape(1, 2), shift.reshape(1, 128))
    return image.reshape(2, 4, BINS)


def solution(mesh):
    return jax.shard_map(
        body,
        mesh=mesh,
        in_specs=(P("blk", "slab", None), P("blk"), P()),
        out_specs=P("blk", "slab", None),
        check_vma=False,
    )
```
